256 devices in a mesh: img: 16 (over x, z_lo, core), patch: 16 (over y, z_hi).
Axes of the slice: x: 4, y: 4, z: 8 (z_hi: 4, z_lo: 2; z = z_hi * 2 + z_lo), core: 2. Of those that a mesh axis runs over, the one named last changes fastest.
Arguments:
- hidden: bfloat16 [32, 16, 128, 640], P('img', 'patch'), may hold values from -100 to 100
- stale_attn_in: bfloat16 [32, 16, 128, 640], P('img', 'patch'), may hold values from -100 to 100
- stale_conv_in: bfloat16 [32, 16, 128, 640], P('img', 'patch'), may hold values from -6 to 6
- ln_gain: float32 [640], replicated, may hold values from 0.25 to 1.75
- ln_bias: float32 [640], replicated, may hold values from -2 to 2
- w_qkv: bfloat16 [640, 1920], replicated, may hold values from -3 to 3
- w_out: bfloat16 [640, 640], replicated, may hold values from -0.25 to 0.25
- gn_gain: float32 [640], replicated, may hold values from 0.25 to 1.75
- gn_bias: float32 [640], replicated, may hold values from -1.5 to 1.5
- conv_weight: bfloat16 [3, 3, 640, 640], replicated, may hold values from -0.078125 to 0.078125
- conv_bias: float32 [640], replicated, may hold values from -1.5 to 1.5
- time_shift: float32 [32, 640], P('img'), may hold values from -6 to 6
Outputs:
- block_out: bfloat16 [32, 16, 128, 640], P('img', 'patch')
The draws below stay inside these ranges and needn't reach their ends.
All inputs are finite; a program needn't handle non-finite values.
Results may differ from the reference program's by a relative error of at most 0.0075.
The reference program's roundings to bfloat16 on the way count: a program that leaves them out, or rounds other values in their place, can miss the bound.
Values may be sent and summed in bfloat16 or wider, within the bound.
No kernel may reach another device: no remote copies, remote signals or barrier semaphores. Data moves between devices by JAX's collectives and lax.ppermute only.
A program may use at most 128 MiB of HBM per device.

```python
import math
import jax
import jax.numpy as jnp
from jax import lax

C = 640
GROUPS = 32
HEAD_DIM = 64
ROWS_DEV = 1
COLS = 128
SAMPLES = 32
ROWS = 16
N_PATCH = 16


def paired_inputs(key):
    base_key = jax.random.fold_in(key, 101)
    subkeys = jax.random.split(base_key, 7)
    full_shape = (SAMPLES, ROWS, COLS, C)
    noise_current = jax.random.truncated_normal(subkeys[0], -4.0, 4.0, full_shape, jnp.float32)
    noise_stale = jax.random.truncated_normal(subkeys[1], -4.0, 4.0, full_shape, jnp.float32)
    pattern = 1.5 * jax.random.truncated_normal(subkeys[6], -4.0, 4.0, (SAMPLES, ROWS, 1, C), jnp.float32)
    row_frac = (jnp.arange(ROWS, dtype=jnp.float32) + 0.5) / ROWS - 0.5
    row_scale = 10.0 ** (row_frac[None, :] + 0.5 * jax.random.uniform(subkeys[2], (SAMPLES, ROWS), jnp.float32) - 0.25)
    col_scale = 2.0 ** (2.0 * jax.random.uniform(subkeys[3], (SAMPLES, COLS), jnp.float32) - 1.0)
    chan_scale = 2.0 ** (2.0 * jax.random.uniform(subkeys[4], (C,), jnp.float32) - 1.0)
    full_scale = row_scale[:, :, None, None] * col_scale[:, None, :, None] * chan_scale
    current = (noise_current + pattern) * full_scale
    stale = (noise_stale + pattern) * full_scale
    current = jnp.clip(current, -96.0, 96.0) * 0.03
    stale = jnp.clip(stale, -96.0, 96.0)
    return (current, stale)


def draw_hidden(key, part):
    return paired_inputs(key)[0].astype(jnp.bfloat16)


def draw_stale_attn_in(key, part):
    return paired_inputs(key)[1].astype(jnp.bfloat16)


def draw_ln_bias(key, part):
    bias_scale = 0.3
    return bias_scale * jax.random.truncated_normal(jax.random.fold_in(key, 303), -4.0, 4.0, (C,), jnp.float32)


def draw_w_qkv(key, part):
    subkeys = jax.random.split(jax.random.fold_in(key, 202), 4)
    query_cols = jax.random.truncated_normal(subkeys[0], -4.0, 4.0, (C, C), jnp.float32) / math.sqrt(C)
    value_cols = jax.random.truncated_normal(subkeys[1], -4.0, 4.0, (C, C), jnp.float32) / math.sqrt(C)
    query_cols = 2.5 * query_cols
    key_cols = jax.random.truncated_normal(subkeys[3], -4.0, 4.0, (C, C), jnp.float32) / math.sqrt(C)
    return jnp.concatenate([query_cols, key_cols, value_cols], 1).astype(jnp.bfloat16)


def block_scale(own_key, extent, pieces, smallest, high):
    factor_of, own = 1.0, jax.random.fold_in(own_key, 6)
    for axis_at, blocks in pieces:
        steps = jnp.exp(jax.random.uniform(jax.random.fold_in(own, axis_at), (blocks,), jnp.float32, smallest / len(pieces), high / len(pieces)))
        factor_of = factor_of * jnp.repeat(steps, extent[axis_at] // blocks).reshape([-1 if axis == axis_at else 1 for axis in range(len(extent))])
    return factor_of


def noise(own_key, shape, scale, reach, cuts=(), kind=jnp.bfloat16):
    drawn = jax.random.normal(own_key, shape, jnp.float32) * scale
    if len(cuts) > 0:
        drawn = block_scale(own_key, shape, cuts, -0.22, 0.18) * drawn
    return jnp.clip(drawn, min=-reach, max=reach).astype(kind)


def setup_inputs(seed: int = 0) -> dict:
    seeds = jax.random.split(jax.random.key(seed), 13)
    return {
        "hidden": draw_hidden(jax.random.fold_in(seeds[12], 71), 0),
        "stale_attn_in": draw_stale_attn_in(jax.random.fold_in(seeds[12], 71), 0),
        "stale_conv_in": noise(seeds[2], (SAMPLES, ROWS, COLS, C), 1.0, 6.0, ((0, 16), (1, 16))),
        "ln_gain": jnp.clip(1.0 + 0.15 * jax.random.normal(seeds[3], (C,), jnp.float32), 0.25, 1.75),
        "ln_bias": draw_ln_bias(jax.random.fold_in(seeds[12], 71), 0),
        "w_qkv": draw_w_qkv(jax.random.fold_in(seeds[12], 71), 0),
        "w_out": noise(seeds[6], (C, C), C ** -0.5, 0.25),
        "gn_gain": jnp.clip(1.0 + 0.15 * jax.random.normal(seeds[7], (C,), jnp.float32), 0.25, 1.75),
        "gn_bias": noise(seeds[8], (C,), 0.3, 1.5, (), jnp.float32),
        "conv_weight": noise(seeds[9], (3, 3, C, C), (9 * C) ** -0.5, 0.078125),
        "conv_bias": noise(seeds[10], (C,), 0.3, 1.5, (), jnp.float32),
        "time_shift": noise(seeds[11], (SAMPLES, C), 1.0, 6.0, ((0, 16),), jnp.float32),
    }


EPSILON = 1e-05

def to_half(values):
    return lax.optimization_barrier(values.astype(jnp.bfloat16))

def layer_norm(values, gain, bias):
    values = values.astype(jnp.float32)
    centre = lax.optimization_barrier(jnp.mean(values, -1, keepdims=True))
    centred = values - centre
    spread = lax.optimization_barrier(jnp.mean(centred * centred, -1, keepdims=True))
    return to_half(centred * lax.rsqrt(spread + EPSILON) * gain + bias)

def reference(hidden, stale_attn_in, stale_conv_in, ln_gain, ln_bias, w_qkv, w_out, gn_gain, gn_bias, conv_weight, conv_bias, time_shift):
    head_count = C // HEAD_DIM
    tokens = ROWS * COLS
    patches = N_PATCH
    per_patch = ROWS_DEV * COLS
    score_scale = HEAD_DIM ** (-0.5)
    fresh_in = layer_norm(hidden, ln_gain, ln_bias).reshape(SAMPLES, tokens, C)
    stale_in = layer_norm(stale_attn_in, ln_gain, ln_bias).reshape(SAMPLES, tokens, C)

    def split_heads(values):
        return values.reshape(patches, per_patch, head_count, HEAD_DIM).transpose(2, 0, 1, 3)

    def one_head(head_parts):
        queries, fresh_keys, fresh_values, stale_keys, stale_values = head_parts
        queries = queries.astype(jnp.float32)
        remote = jnp.einsum('pqd,rkd->pqrk', queries, stale_keys.astype(jnp.float32)) * score_scale
        local_scores = jnp.einsum('pqd,pkd->pqk', queries, fresh_keys.astype(jnp.float32)) * score_scale
        same_patch = jnp.eye(patches, dtype=bool)[:, None, :, None]
        remote = jnp.where(same_patch, -jnp.inf, remote)
        row_max = jnp.maximum(lax.optimization_barrier(jnp.max(remote, axis=(2, 3))), lax.optimization_barrier(jnp.max(local_scores, -1)))
        remote_weights = jnp.exp(remote - row_max[:, :, None, None])
        local_weights = jnp.exp(local_scores - row_max[:, :, None])
        weight_sum = lax.optimization_barrier(jnp.sum(remote_weights, axis=(2, 3))) + lax.optimization_barrier(jnp.sum(local_weights, -1))
        gathered = jnp.einsum('pqrk,rkd->pqd', to_half(remote_weights).astype(jnp.float32), stale_values.astype(jnp.float32))
        gathered = gathered + jnp.einsum('pqk,pkd->pqd', to_half(local_weights).astype(jnp.float32), fresh_values.astype(jnp.float32))
        return gathered / weight_sum[:, :, None]

    def attend_sample(operands):
        fresh_rows, stale_rows = operands
        projected = to_half(jnp.dot(fresh_rows, w_qkv, preferred_element_type=jnp.float32))
        stale_pairs = to_half(jnp.dot(stale_rows, w_qkv[:, C:], preferred_element_type=jnp.float32))
        head_parts = (split_heads(projected[:, :C]), split_heads(projected[:, C:2 * C]), split_heads(projected[:, 2 * C:]), split_heads(stale_pairs[:, :C]), split_heads(stale_pairs[:, C:]))
        per_head = lax.map(one_head, head_parts)
        attended = to_half(per_head.transpose(1, 2, 0, 3).reshape(tokens, C))
        return jnp.dot(attended, w_out, preferred_element_type=jnp.float32)
    attention_out = lax.map(attend_sample, (fresh_in, stale_in))
    residual = to_half(hidden.reshape(SAMPLES, tokens, C).astype(jnp.float32) + attention_out)
    grouped = residual.astype(jnp.float32).reshape(SAMPLES, tokens, GROUPS, C // GROUPS)
    group_mean = lax.optimization_barrier(jnp.mean(grouped, axis=(1, 3), keepdims=True))
    centred = grouped - group_mean
    group_var = lax.optimization_barrier(jnp.mean(centred * centred, axis=(1, 3), keepdims=True))
    normalized = (centred * lax.rsqrt(group_var + EPSILON)).reshape(SAMPLES, tokens, C)
    activated = to_half(jax.nn.silu(normalized * gn_gain + gn_bias)).reshape(SAMPLES, ROWS, COLS, C)

    def convolve(operands):
        fresh_rows, stale_rows = operands
        fresh_patch = fresh_rows.reshape(patches, ROWS_DEV, COLS, C)
        stale_patch = stale_rows.reshape(patches, ROWS_DEV, COLS, C)
        zero_rim = jnp.zeros((1, 1, COLS, C), jnp.bfloat16)
        rim_above = jnp.concatenate([zero_rim, stale_patch[:-1, ROWS_DEV - 1:]], 0)
        rim_below = jnp.concatenate([stale_patch[1:, :1], zero_rim], 0)
        framed = jnp.concatenate([rim_above, fresh_patch, rim_below], 1)
        framed = jnp.pad(framed, ((0, 0), (0, 0), (1, 1), (0, 0)))
        summed = jnp.zeros((patches * ROWS_DEV * COLS, C), jnp.float32)
        for tap_row in range(3):
            for tap_col in range(3):
                window = framed[:, tap_row:tap_row + ROWS_DEV, tap_col:tap_col + COLS, :].reshape(-1, C)
                summed = summed + jnp.dot(window, conv_weight[tap_row, tap_col], preferred_element_type=jnp.float32)
        return summed.reshape(ROWS, COLS, C)
    convolved = lax.map(convolve, (activated, stale_conv_in))
    summed_out = convolved + conv_bias + time_shift[:, None, None, :] + residual.astype(jnp.float32).reshape(SAMPLES, ROWS, COLS, C)
    return summed_out.astype(jnp.bfloat16)
```

```python
import functools

import jax
import jax.numpy as jnp
import numpy as np
from jax import lax
from jax.experimental import pallas as pl
from jax.experimental.pallas import tpu as pltpu
from jax.sharding import Mesh
from jax.sharding import PartitionSpec as P

GROUPS = 32
HEAD_DIM = 64
EPSILON = 1e-05
LANES = 128
PIECES = 8


F32 = jnp.float32
BF16 = jnp.bfloat16


def normalize(values, gain, bias):
    values = values.astype(F32)
    centre = jnp.mean(values, -1, keepdims=True)
    centred = values - centre
    spread = jnp.mean(centred * centred, -1, keepdims=True)
    return (centred * lax.rsqrt(spread + EPSILON) * gain + bias).astype(BF16)


def as_row(ref):
    return ref[...].reshape(1, -1)


def stale_norm_kernel(x_ref, gain_ref, bias_ref, *out_refs):
    rows = out_refs[0].shape[0]
    gain, bias = as_row(gain_ref), as_row(bias_ref)
    for index, out_ref in enumerate(out_refs):
        out_ref[...] = normalize(x_ref[index * rows : (index + 1) * rows, :], gain, bias)


def query_kernel(x_ref, gain_ref, bias_ref, w_ref, *out_refs):
    normed = normalize(x_ref[...], as_row(gain_ref), as_row(bias_ref))
    projected = jnp.dot(normed, w_ref[...], preferred_element_type=F32).astype(BF16)
    scaled = (projected.astype(F32) * HEAD_DIM ** (-0.5)).astype(BF16)
    rows = out_refs[0].shape[0]
    half = len(out_refs) // 2
    for index in range(half):
        part = slice(index * rows, (index + 1) * rows)
        out_refs[index][...] = scaled[part]
        out_refs[half + index][...] = normed[part]


def scores_of(queries, keys):
    return lax.dot_general(
        queries, keys, (((1,), (1,)), ((), ())), preferred_element_type=F32
    )


def attend_kernel(
    q0_ref, q1_ref, q2_ref, q3_ref,
    z1_ref, z2_ref, z3_ref, fresh_ref, own_ref,
    wk_ref, wv_ref,
    o0_ref, o1_ref, o2_ref, o3_ref,
    x_scr, tile_scr,
):
    pair = pl.program_id(0)
    rows = fresh_ref.shape[0]
    channels = fresh_ref.shape[1]
    out_refs = (o0_ref, o1_ref, o2_ref, o3_ref)

    @pl.when(pair == 0)
    def _():
        for index, ref in enumerate((z1_ref, z2_ref, z3_ref, fresh_ref, own_ref)):
            x_scr[index * rows : (index + 1) * rows, :] = ref[...]
        tile_scr[...] = jnp.zeros_like(tile_scr)

    weights = jnp.concatenate([wk_ref[...], wv_ref[...]], axis=1)
    pairs = jnp.dot(x_scr[...], weights, preferred_element_type=F32).astype(BF16)
    keys, values = pairs[:, :LANES], pairs[:, LANES:]
    low_all = lax.broadcasted_iota(jnp.int32, keys.shape, 1) < HEAD_DIM
    zero = jnp.zeros((), BF16)
    one = jnp.ones((), BF16)
    low_values = jnp.concatenate(
        [jnp.where(low_all, values, zero), jnp.where(low_all, one, zero)], axis=1
    )
    high_values = jnp.concatenate(
        [jnp.where(low_all, zero, values), jnp.where(low_all, zero, one)], axis=1
    )
    common, fresh, own = slice(0, 3 * rows), slice(3 * rows, 4 * rows), slice(4 * rows, 5 * rows)
    queries = jnp.concatenate([q0_ref[...], q1_ref[...], q2_ref[...], q3_ref[...]], 0)
    lane = lax.broadcasted_iota(jnp.int32, queries.shape, 1)
    low = lane < HEAD_DIM
    shared_weights, single_weights, tops = [], [], []
    for part in (jnp.where(low, queries, zero), jnp.where(low, zero, queries)):
        shared = scores_of(part, keys[common])
        single = jnp.concatenate(
            [scores_of(part[:rows], keys[fresh]), scores_of(part[rows:], keys[own])], 0
        )
        top = single
        for index in range(3):
            top = jnp.maximum(top, shared[:, index * LANES : (index + 1) * LANES])
        top = jnp.max(top, -1, keepdims=True)
        tops.append(top)
        shared_weights.append(jnp.exp(shared - top).astype(BF16))
        single_weights.append(jnp.exp(single - top).astype(BF16))
    summed = jnp.dot(
        jnp.concatenate(shared_weights, 1),
        jnp.concatenate([low_values[common], high_values[common]], 0),
        preferred_element_type=F32,
    )
    single = jnp.concatenate(single_weights, 1)
    summed = summed + jnp.concatenate(
        [
            jnp.dot(
                single[:rows],
                jnp.concatenate([low_values[fresh], high_values[fresh]], 0),
                preferred_element_type=F32,
            ),
            jnp.dot(
                single[rows:],
                jnp.concatenate([low_values[own], high_values[own]], 0),
                preferred_element_type=F32,
            ),
        ],
        0,
    )
    total = summed[:, LANES:]
    mixed = (summed[:, :LANES] / total).astype(BF16)
    lanes = pl.ds(pl.multiple_of(pair * LANES, LANES), LANES)
    for index, o_ref in enumerate(out_refs):
        o_ref[:, lanes] = mixed[index * rows : (index + 1) * rows]
    rest = jnp.where(low, tops[0], tops[1]) + jnp.log(total)
    slot = lane & (HEAD_DIM - 1)
    tile = tile_scr[...]
    for piece in range(3):
        rounded = rest.astype(BF16).astype(F32)
        tile = jnp.where(slot == pair + piece * PIECES, rounded, tile)
        rest = rest - rounded
    tile_scr[...] = tile

    @pl.when(pair == pl.num_programs(0) - 1)
    def _():
        for index, o_ref in enumerate(out_refs):
            o_ref[:, channels:] = tile_scr[index * rows : (index + 1) * rows, :].astype(BF16)


def spread_matrix(channels):
    out = np.zeros((LANES, channels), np.float32)
    for channel in range(channels):
        head = channel // HEAD_DIM
        base = (head % 2) * HEAD_DIM + head // 2
        for piece in range(3):
            out[base + piece * PIECES, channel] = 1
    return out


def exact_dot(x, ones):
    total = None
    for _ in range(3):
        rounded = x.astype(BF16)
        part = jnp.dot(rounded, ones, preferred_element_type=F32)
        total = part if total is None else total + part
        x = x - rounded.astype(F32)
    return total


def merge_kernel(
    o0_ref, o1_ref, o2_ref, o3_ref, hidden_ref, w_ref, spread_ref, gather_ref, *rest_refs, sample
):
    channels = hidden_ref.shape[1]
    rows = hidden_ref.shape[0]
    refs = (o0_ref, o1_ref, o2_ref, o3_ref)
    tiles = jnp.concatenate([ref[:, channels:] for ref in refs], 0)
    logs = jnp.dot(tiles, spread_ref[...], preferred_element_type=F32)
    logs = [logs[index * rows : (index + 1) * rows] for index in range(4)]
    top = jnp.maximum(jnp.maximum(logs[0], logs[1]), jnp.maximum(logs[2], logs[3]))
    numer = denom = None
    for ref, one in zip(refs, logs):
        factor = jnp.exp(one - top)
        upper = factor * ref[:, :channels].astype(F32)
        numer, denom = (upper, factor) if numer is None else (numer + upper, denom + factor)
    attended = (numer / denom).astype(BF16)
    residual = (
        hidden_ref[...].astype(F32) + jnp.dot(attended, w_ref[...], preferred_element_type=F32)
    ).astype(BF16)
    res_ref, stat_ref = rest_refs[-2:]
    res_ref[...] = residual
    wide = residual.astype(F32)
    sums = jnp.concatenate(
        [jnp.sum(wide, 0, keepdims=True), jnp.sum(wide * wide, 0, keepdims=True)]
        + [jnp.zeros((6, channels), F32)],
        0,
    )
    sums = exact_dot(sums, gather_ref[...])
    if sample:
        sums = pltpu.roll(sums, 2 * sample, 0) + rest_refs[0][...]
        stat_ref[...] = jnp.broadcast_to(sums[None], stat_ref.shape)
    else:
        stat_ref[...] = sums


def shifted(x, by, cols):
    rolled = pltpu.roll(x, by % x.shape[0], 0)
    col = lax.broadcasted_iota(jnp.int32, x.shape, 0) & (cols - 1)
    edge = 0 if by == 1 else cols - 1
    return jnp.where(col == edge, 0.0, rolled).astype(BF16)


def taps(x, w_ref, cols):
    wide = x.astype(F32)
    total = jnp.dot(shifted(wide, 1, cols), w_ref[0], preferred_element_type=F32)
    total += jnp.dot(x, w_ref[1], preferred_element_type=F32)
    total += jnp.dot(shifted(wide, -1, cols), w_ref[2], preferred_element_type=F32)
    return total


def rim_kernel(above_ref, below_ref, w_ref, bias_ref, shift_ref, out_ref, *, cols):
    step = pl.program_id(0)

    @pl.when(step == 0)
    def _():
        first = taps(above_ref[...], w_ref, cols) + as_row(bias_ref)
        samples = first.shape[0] // cols
        for sample in range(samples):
            part = slice(sample * cols, (sample + 1) * cols)
            out_ref[part, :] = first[part] + shift_ref[sample : sample + 1, :]

    @pl.when(step == 1)
    def _():
        out_ref[...] += taps(below_ref[...], w_ref, cols)


def final_kernel(
    res0_ref, res1_ref, stat_ref, gain_ref, bias_ref, scatter_ref, w_ref, rim_ref, out_ref,
    *, cols, cells
):
    activated = []
    wide = []
    sums = exact_dot(jnp.sum(stat_ref[...], 0), scatter_ref[...])
    gain, bias = as_row(gain_ref), as_row(bias_ref)
    for sample, res_ref in enumerate((res0_ref, res1_ref)):
        mean = sums[2 * sample : 2 * sample + 1] / cells
        var = sums[2 * sample + 1 : 2 * sample + 2] / cells - mean * mean
        residual = res_ref[...].astype(F32)
        wide.append(residual)
        normalized = (residual - mean) * lax.rsqrt(var + EPSILON)
        value = normalized * gain + bias
        activated.append((value / (1.0 + jnp.exp(-value))).astype(BF16))
    x = jnp.concatenate(activated, 0)
    out_ref[...] = (
        taps(x, w_ref, cols) + rim_ref[...] + jnp.concatenate(wide, 0)
    ).astype(BF16)


def ring(by, count):
    return [(i, (i + by) % count) for i in range(count)]


def call(kernel, out_shape, *args, flops=1000000, **kwargs):
    return pl.pallas_call(
        kernel,
        out_shape=out_shape,
        cost_estimate=pl.CostEstimate(flops=flops, bytes_accessed=1000000, transcendentals=0),
        **kwargs,
    )(*args)


def shards(
    hidden, stale_attn_in, stale_conv_in, ln_gain, ln_bias, w_qkv, w_out,
    gn_gain, gn_bias, conv_weight, conv_bias, time_shift,
):
    samples, rows_dev, cols, channels = hidden.shape
    tokens = rows_dev * cols
    every = samples * tokens
    pair_count = channels // LANES
    y_count, z_count = lax.axis_size("y"), lax.axis_size("z")
    count = y_count * z_count
    hid = hidden.reshape(every, channels)
    block = jax.ShapeDtypeStruct((tokens, channels), BF16)
    full = pl.BlockSpec((every, channels), lambda i: (0, 0))
    vector = pl.BlockSpec((channels,), lambda i: (0,))
    whole = pl.BlockSpec((tokens, channels), lambda i: (0, 0))
    shifts = (1, 3, 2)

    stale = call(
        stale_norm_kernel, [block] * samples,
        stale_attn_in.reshape(every, channels), ln_gain, ln_bias,
    )
    along = [[lax.ppermute(one, "z", ring(by, z_count)) for by in shifts] for one in stale]
    outs = call(
        query_kernel, [block] * (2 * samples), hid, ln_gain, ln_bias, w_qkv,
        grid=(1,),
        in_specs=[full, vector, vector, pl.BlockSpec((channels, channels), lambda i: (0, 0))],
        out_specs=[whole] * (2 * samples),
        flops=2 * every * channels * channels,
    )
    queries, fresh = outs[:samples], outs[samples:]
    all_queries = [
        [one] + [lax.ppermute(one, "y", ring(by, y_count)) for by in shifts]
        for one in queries
    ]
    conv_rows = stale_conv_in.reshape(every, channels)
    above = lax.ppermute(conv_rows, ("y", "z"), [(i, i + 1) for i in range(count - 1)])
    below = lax.ppermute(conv_rows, ("y", "z"), [(i + 1, i) for i in range(count - 1)])

    wide = channels + LANES
    spread = jnp.asarray(spread_matrix(channels), BF16)
    group = np.arange(channels) // (channels // GROUPS)
    gather = group[:, None] == np.arange(LANES)[None, :]
    ext = jax.ShapeDtypeStruct((tokens, wide), BF16)
    back = []
    for s in range(samples):
        outs = call(
            attend_kernel, [ext] * 4,
            *all_queries[s], along[s][0], along[s][2], along[s][1], fresh[s], stale[s],
            w_qkv, w_qkv,
            grid=(pair_count,),
            in_specs=[pl.BlockSpec((tokens, LANES), lambda p: (0, p))] * 4
            + [whole] * 5
            + [
                pl.BlockSpec((channels, LANES), lambda p: (0, pair_count + p)),
                pl.BlockSpec((channels, LANES), lambda p: (0, 2 * pair_count + p)),
            ],
            out_specs=[pl.BlockSpec((tokens, wide), lambda p: (0, 0))] * 4,
            scratch_shapes=[
                pltpu.VMEM((5 * tokens, channels), BF16),
                pltpu.VMEM((4 * tokens, LANES), F32),
            ],
            flops=6 * 10 ** 9,
        )
        back.append(
            [outs[0]]
            + [lax.ppermute(one, "y", ring(-by, y_count)) for one, by in zip(outs[1:], shifts)]
        )
    rim = call(
        functools.partial(rim_kernel, cols=cols),
        jax.ShapeDtypeStruct((every, channels), F32),
        above, below, conv_weight, conv_bias, time_shift,
        grid=(2,),
        in_specs=[
            full, full,
            pl.BlockSpec((None, 3, channels, channels), lambda i: (2 * i, 0, 0, 0)),
            vector,
            pl.BlockSpec((samples, channels), lambda i: (0, 0)),
        ],
        out_specs=full,
        flops=12 * every * channels * channels,
    )
    residuals, stats = [], []
    for s in range(samples):
        small = jax.ShapeDtypeStruct((8, LANES), F32)
        if s:
            small = jax.ShapeDtypeStruct((count, 8, LANES), F32)
        res, stat = call(
            functools.partial(merge_kernel, sample=s), [block, small],
            *back[s], hid, w_out, spread, jnp.asarray(gather, BF16), *stats,
            grid=(1,),
            in_specs=[pl.BlockSpec((tokens, wide), lambda i: (0, 0))] * 4
            + [
                pl.BlockSpec((tokens, channels), lambda i, s=s: (s, 0)),
                pl.BlockSpec((channels, channels), lambda i: (0, 0)),
                pl.BlockSpec((LANES, channels), lambda i: (0, 0)),
                pl.BlockSpec((channels, LANES), lambda i: (0, 0)),
            ]
            + [pl.BlockSpec((8, LANES), lambda i: (0, 0))] * len(stats),
            out_specs=[whole, pl.BlockSpec(small.shape, lambda i, n=small.ndim: (0,) * n)],
            flops=10 ** 9,
        )
        residuals.append(res)
        stats = [stat]
    shared = lax.all_to_all(stats[0], ("y", "z"), 0, 0)
    out = call(
        functools.partial(
            final_kernel, cols=cols, cells=float(count * tokens * (channels // GROUPS))
        ),
        jax.ShapeDtypeStruct((every, channels), BF16),
        *residuals, shared, gn_gain, gn_bias, jnp.asarray(gather.T, BF16), conv_weight, rim,
        grid=(1,),
        in_specs=[
            whole, whole,
            pl.BlockSpec((count, 8, LANES), lambda i: (0, 0, 0)),
            vector, vector,
            pl.BlockSpec((LANES, channels), lambda i: (0, 0)),
            pl.BlockSpec((None, 3, channels, channels), lambda i: (1, 0, 0, 0)),
            full,
        ],
        out_specs=full,
        flops=6 * every * channels * channels,
    )
    return out.reshape(hidden.shape)


def solution(mesh):
    split = Mesh(mesh.devices.reshape(mesh.shape["img"], 4, 4), ("img", "y", "z"))
    rows = P("img", ("y", "z"), None, None)

    return jax.shard_map(
        shards,
        mesh=split,
        in_specs=(rows, rows, rows, P(), P(), P(), P(), P(), P(), P(), P(), P("img", None)),
        out_specs=rows,
        check_vma=False,
    )
```

```python
import functools

import jax
import jax.numpy as jnp
import numpy as np
from jax import lax
from jax.experimental import pallas as pl
from jax.experimental.pallas import tpu as pltpu
from jax.sharding import Mesh
from jax.sharding import PartitionSpec as P

GROUPS = 32
HEAD_DIM = 64
EPSILON = 1e-05
LANES = 128
PIECES = 8


F32 = jnp.float32
BF16 = jnp.bfloat16
VMEM = pl.BlockSpec(memory_space=pltpu.VMEM)


def normalize(values, gain, bias):
    values = values.astype(F32)
    centre = jnp.mean(values, -1, keepdims=True)
    centred = values - centre
    spread = jnp.mean(centred * centred, -1, keepdims=True)
    return (centred * lax.rsqrt(spread + EPSILON) * gain + bias).astype(BF16)


def as_row(ref):
    return ref[...].reshape(1, -1)


def stale_norm_kernel(x_ref, gain_ref, bias_ref, *out_refs):
    rows = out_refs[0].shape[0]
    gain, bias = as_row(gain_ref), as_row(bias_ref)
    for index, out_ref in enumerate(out_refs):
        out_ref[...] = normalize(x_ref[index * rows : (index + 1) * rows, :], gain, bias)


def query_kernel(x_ref, gain_ref, bias_ref, w_ref, *out_refs):
    normed = normalize(x_ref[...], as_row(gain_ref), as_row(bias_ref))
    projected = jnp.dot(normed, w_ref[...], preferred_element_type=F32).astype(BF16)
    scaled = (projected.astype(F32) * HEAD_DIM ** (-0.5)).astype(BF16)
    rows = out_refs[0].shape[0]
    half = len(out_refs) // 2
    for index in range(half):
        part = slice(index * rows, (index + 1) * rows)
        out_refs[index][...] = scaled[part]
        out_refs[half + index][...] = normed[part]


def scores_of(queries, keys):
    return lax.dot_general(
        queries, keys, (((1,), (1,)), ((), ())), preferred_element_type=F32
    )


def project(x, wk_ref, wv_ref, kv_scr, slot):
    weights = jnp.concatenate([wk_ref[...], wv_ref[...]], axis=1)
    kv_scr[slot] = jnp.dot(x, weights, preferred_element_type=F32).astype(BF16)


def attend_kernel(
    q0_ref, q1_ref, q2_ref, q3_ref,
    z1_ref, z2_ref, z3_ref, fresh_ref, own_ref,
    wk0_ref, wv0_ref, wk_ref, wv_ref,
    o0_ref, o1_ref, o2_ref, o3_ref,
    x_scr, kv_scr, tile_scr,
):
    pair = pl.program_id(0)
    rows = fresh_ref.shape[0]
    channels = fresh_ref.shape[1]
    out_refs = (o0_ref, o1_ref, o2_ref, o3_ref)

    @pl.when(pair == 0)
    def _():
        for index, ref in enumerate((z1_ref, z2_ref, z3_ref, fresh_ref, own_ref)):
            x_scr[index * rows : (index + 1) * rows, :] = ref[...]
        tile_scr[...] = jnp.zeros_like(tile_scr)
        project(x_scr[...], wk0_ref, wv0_ref, kv_scr, 0)

    current = pair & 1
    keys, values = kv_scr[current, :, :LANES], kv_scr[current, :, LANES:]
    low_all = lax.broadcasted_iota(jnp.int32, keys.shape, 1) < HEAD_DIM
    zero = jnp.zeros((), BF16)
    one = jnp.ones((), BF16)
    low_values = jnp.concatenate(
        [jnp.where(low_all, values, zero), jnp.where(low_all, one, zero)], axis=1
    )
    high_values = jnp.concatenate(
        [jnp.where(low_all, zero, values), jnp.where(low_all, zero, one)], axis=1
    )
    common, fresh, own = slice(0, 3 * rows), slice(3 * rows, 4 * rows), slice(4 * rows, 5 * rows)
    lanes = pl.ds(pl.multiple_of(pair * LANES, LANES), LANES)
    mine = q0_ref[:, lanes]
    others = jnp.concatenate([q1_ref[:, lanes], q2_ref[:, lanes], q3_ref[:, lanes]], 0)

    def halves(x):
        low_part = lax.broadcasted_iota(jnp.int32, x.shape, 1) < HEAD_DIM
        return jnp.concatenate([jnp.where(low_part, x, zero), jnp.where(low_part, zero, x)], 0)

    mine, others = halves(mine), halves(others)
    shared = scores_of(jnp.concatenate([mine, others], 0), keys[common])
    single = jnp.concatenate([scores_of(mine, keys[fresh]), scores_of(others, keys[own])], 0)
    top = single
    for index in range(3):
        top = jnp.maximum(top, shared[:, index * LANES : (index + 1) * LANES])
    top = jnp.max(top, -1, keepdims=True)
    shared = jnp.exp(shared - top).astype(BF16)
    single = jnp.exp(single - top).astype(BF16)

    def paired(x):
        return (
            jnp.concatenate([x[:rows], x[2 * rows : 5 * rows]], 0),
            jnp.concatenate([x[rows : 2 * rows], x[5 * rows :]], 0),
        )

    summed = jnp.dot(
        jnp.concatenate(paired(shared), 1),
        jnp.concatenate([low_values[common], high_values[common]], 0),
        preferred_element_type=F32,
    )
    single = jnp.concatenate(paired(single), 1)
    summed = summed + jnp.concatenate(
        [
            jnp.dot(
                single[:rows],
                jnp.concatenate([low_values[fresh], high_values[fresh]], 0),
                preferred_element_type=F32,
            ),
            jnp.dot(
                single[rows:],
                jnp.concatenate([low_values[own], high_values[own]], 0),
                preferred_element_type=F32,
            ),
        ],
        0,
    )
    total = summed[:, LANES:]
    mixed = (summed[:, :LANES] / total).astype(BF16)
    for index, o_ref in enumerate(out_refs):
        o_ref[:, lanes] = mixed[index * rows : (index + 1) * rows]
    lane = lax.broadcasted_iota(jnp.int32, total.shape, 1)
    low_top, high_top = paired(top)
    rest = jnp.where(lane < HEAD_DIM, low_top, high_top) + jnp.log(total)
    slot = lane & (HEAD_DIM - 1)
    tile = tile_scr[...]
    for piece in range(3):
        rounded = rest.astype(BF16).astype(F32)
        tile = jnp.where(slot == pair + piece * PIECES, rounded, tile)
        rest = rest - rounded
    tile_scr[...] = tile
    project(x_scr[...], wk_ref, wv_ref, kv_scr, 1 - current)

    @pl.when(pair == pl.num_programs(0) - 1)
    def _():
        for index, o_ref in enumerate(out_refs):
            o_ref[:, channels:] = tile_scr[index * rows : (index + 1) * rows, :].astype(BF16)


def spread_matrix(channels):
    out = np.zeros((LANES, channels), np.float32)
    for channel in range(channels):
        head = channel // HEAD_DIM
        base = (head % 2) * HEAD_DIM + head // 2
        for piece in range(3):
            out[base + piece * PIECES, channel] = 1
    return out


def exact_dot(x, ones):
    total = None
    for _ in range(3):
        rounded = x.astype(BF16)
        part = jnp.dot(rounded, ones, preferred_element_type=F32)
        total = part if total is None else total + part
        x = x - rounded.astype(F32)
    return total


def merge_kernel(
    o0_ref, o1_ref, o2_ref, o3_ref, hidden_ref, w_ref, spread_ref, gather_ref, *rest_refs, sample
):
    channels = hidden_ref.shape[1]
    rows = hidden_ref.shape[0]
    refs = (o0_ref, o1_ref, o2_ref, o3_ref)
    tiles = jnp.concatenate([ref[:, channels:] for ref in refs], 0)
    logs = jnp.dot(tiles, spread_ref[...], preferred_element_type=F32)
    logs = [logs[index * rows : (index + 1) * rows] for index in range(4)]
    top = jnp.maximum(jnp.maximum(logs[0], logs[1]), jnp.maximum(logs[2], logs[3]))
    numer = denom = None
    for ref, one in zip(refs, logs):
        factor = jnp.exp(one - top)
        upper = factor * ref[:, :channels].astype(F32)
        numer, denom = (upper, factor) if numer is None else (numer + upper, denom + factor)
    attended = (numer / denom).astype(BF16)
    residual = (
        hidden_ref[...].astype(F32) + jnp.dot(attended, w_ref[...], preferred_element_type=F32)
    ).astype(BF16)
    res_ref, stat_ref = rest_refs[-2:]
    res_ref[...] = residual
    wide = residual.astype(F32)
    sums = jnp.concatenate(
        [jnp.sum(wide, 0, keepdims=True), jnp.sum(wide * wide, 0, keepdims=True)]
        + [jnp.zeros((6, channels), F32)],
        0,
    )
    sums = exact_dot(sums, gather_ref[...])
    if sample:
        sums = pltpu.roll(sums, 2 * sample, 0) + rest_refs[0][...]
        stat_ref[...] = jnp.broadcast_to(sums[None], stat_ref.shape)
    else:
        stat_ref[...] = sums


def shifted(x, by, cols):
    rolled = pltpu.roll(x, by % x.shape[0], 0)
    col = lax.broadcasted_iota(jnp.int32, x.shape, 0) & (cols - 1)
    edge = 0 if by == 1 else cols - 1
    return jnp.where(col == edge, 0.0, rolled).astype(BF16)


def taps(x, weights, cols):
    wide = x.astype(F32)
    unfolded = jnp.concatenate([shifted(wide, 1, cols), x, shifted(wide, -1, cols)], 1)
    weights = weights.reshape(-1, weights.shape[-1])
    return jnp.dot(unfolded, weights, preferred_element_type=F32)


def rim_kernel(above_ref, below_ref, w_ref, bias_ref, shift_ref, out_ref, *, cols):
    total = taps(above_ref[...], w_ref[0], cols) + taps(below_ref[...], w_ref[2], cols)
    total += as_row(bias_ref)
    for sample in range(total.shape[0] // cols):
        part = slice(sample * cols, (sample + 1) * cols)
        out_ref[part, :] = total[part] + shift_ref[sample : sample + 1, :]


def final_kernel(
    res0_ref, res1_ref, stat_ref, gain_ref, bias_ref, scatter_ref, w_ref, rim_ref, out_ref,
    *, cols, cells
):
    activated = []
    wide = []
    sums = exact_dot(jnp.sum(stat_ref[...], 0), scatter_ref[...])
    gain, bias = as_row(gain_ref), as_row(bias_ref)
    for sample, res_ref in enumerate((res0_ref, res1_ref)):
        mean = sums[2 * sample : 2 * sample + 1] / cells
        var = sums[2 * sample + 1 : 2 * sample + 2] / cells - mean * mean
        residual = res_ref[...].astype(F32)
        wide.append(residual)
        normalized = (residual - mean) * lax.rsqrt(var + EPSILON)
        value = normalized * gain + bias
        activated.append((value / (1.0 + jnp.exp(-value))).astype(BF16))
    x = jnp.concatenate(activated, 0)
    out_ref[...] = (
        taps(x, w_ref[1], cols) + rim_ref[...] + jnp.concatenate(wide, 0)
    ).astype(BF16)


def ring(by, count):
    return [(i, (i + by) % count) for i in range(count)]


def on_chip(x):
    return pltpu.with_memory_space_constraint(x, pltpu.VMEM)


def call(kernel, out_shape, *args, flops=1000000, chip=(), **kwargs):
    args = [on_chip(x) if index in chip else x for index, x in enumerate(args)]
    return pl.pallas_call(
        kernel,
        out_shape=out_shape,
        compiler_params=pltpu.CompilerParams(vmem_limit_bytes=24 * 2 ** 20),
        cost_estimate=pl.CostEstimate(flops=flops, bytes_accessed=1000000, transcendentals=0),
        **kwargs,
    )(*args)


def shards(
    hidden, stale_attn_in, stale_conv_in, ln_gain, ln_bias, w_qkv, w_out,
    gn_gain, gn_bias, conv_weight, conv_bias, time_shift,
):
    samples, rows_dev, cols, channels = hidden.shape
    tokens = rows_dev * cols
    every = samples * tokens
    pair_count = channels // LANES
    y_count, z_count = lax.axis_size("y"), lax.axis_size("z")
    count = y_count * z_count
    hid = hidden.reshape(every, channels)
    block = pltpu.VMEM((tokens, channels), BF16)
    full = pl.BlockSpec((every, channels), lambda i: (0, 0))
    shifts = (1, 3, 2)

    stale = call(
        stale_norm_kernel, [block] * samples,
        stale_attn_in.reshape(every, channels), ln_gain, ln_bias,
        in_specs=[VMEM] * 3, out_specs=[VMEM] * samples,
    )
    along = [[lax.ppermute(one, "z", ring(by, z_count)) for by in shifts] for one in stale]
    outs = call(
        query_kernel, [block] * (2 * samples), hid, ln_gain, ln_bias, w_qkv,
        grid=(1,),
        in_specs=[VMEM, VMEM, VMEM, pl.BlockSpec((channels, channels), lambda i: (0, 0))],
        out_specs=[VMEM] * (2 * samples),
        flops=2 * every * channels * channels,
    )
    queries, fresh = outs[:samples], outs[samples:]
    all_queries = [
        [one] + [lax.ppermute(one, "y", ring(by, y_count)) for by in shifts]
        for one in queries
    ]
    conv_rows = stale_conv_in.reshape(every, channels)
    above = lax.ppermute(conv_rows, ("y", "z"), [(i, i + 1) for i in range(count - 1)])
    below = lax.ppermute(conv_rows, ("y", "z"), [(i + 1, i) for i in range(count - 1)])

    wide = channels + LANES
    spread = jnp.asarray(spread_matrix(channels), BF16)
    group = np.arange(channels) // (channels // GROUPS)
    gather = group[:, None] == np.arange(LANES)[None, :]
    ext = pltpu.VMEM((tokens, wide), BF16)
    back = []
    for s in range(samples):
        outs = call(
            attend_kernel, [ext] * 4,
            *all_queries[s], along[s][0], along[s][2], along[s][1], fresh[s], stale[s],
            w_qkv, w_qkv, w_qkv, w_qkv,
            grid=(pair_count,),
            in_specs=[VMEM] * 9
            + [
                pl.BlockSpec((channels, LANES), lambda p: (0, pair_count)),
                pl.BlockSpec((channels, LANES), lambda p: (0, 2 * pair_count)),
                pl.BlockSpec((channels, LANES), lambda p: (0, jnp.minimum(pair_count + p + 1, 2 * pair_count - 1))),
                pl.BlockSpec((channels, LANES), lambda p: (0, jnp.minimum(2 * pair_count + p + 1, 3 * pair_count - 1))),
            ],
            out_specs=[VMEM] * 4,
            scratch_shapes=[
                pltpu.VMEM((5 * tokens, channels), BF16),
                pltpu.VMEM((2, 5 * tokens, 2 * LANES), BF16),
                pltpu.VMEM((4 * tokens, LANES), F32),
            ],
            flops=6 * 10 ** 9,
            chip=range(9),
        )
        back.append(
            [outs[0]]
            + [lax.ppermute(one, "y", ring(-by, y_count)) for one, by in zip(outs[1:], shifts)]
        )
    rim = call(
        functools.partial(rim_kernel, cols=cols),
        pltpu.VMEM((every, channels), F32),
        above, below, conv_weight, conv_bias, time_shift,
        in_specs=[VMEM] * 5,
        out_specs=VMEM,
        flops=12 * every * channels * channels,
        chip=(0, 1, 2),
    )
    residuals, stats = [], []
    for s in range(samples):
        small = pltpu.VMEM((8, LANES), F32)
        if s:
            small = pltpu.VMEM((count, 8, LANES), F32)
        res, stat = call(
            functools.partial(merge_kernel, sample=s), [block, small],
            *back[s], hid, w_out, spread, jnp.asarray(gather, BF16), *stats,
            grid=(1,),
            in_specs=[VMEM] * 4
            + [pl.BlockSpec((tokens, channels), lambda i, s=s: (s, 0))]
            + [VMEM] * (3 + len(stats)),
            out_specs=[VMEM, VMEM],
            flops=10 ** 9,
            chip=(0, 1, 2, 3, 5) + (8,) * s,
        )
        residuals.append(res)
        stats = [stat]
    shared = lax.all_to_all(stats[0], ("y", "z"), 0, 0)
    out = call(
        functools.partial(
            final_kernel, cols=cols, cells=float(count * tokens * (channels // GROUPS))
        ),
        jax.ShapeDtypeStruct((every, channels), BF16),
        *residuals, shared, gn_gain, gn_bias, jnp.asarray(gather.T, BF16), conv_weight, rim,
        in_specs=[VMEM] * 8,
        out_specs=VMEM,
        chip=(0, 1, 2, 6, 7),
        flops=6 * every * channels * channels,
    )
    return out.reshape(hidden.shape)


def solution(mesh):
    split = Mesh(mesh.devices.reshape(mesh.shape["img"], 4, 4), ("img", "y", "z"))
    rows = P("img", ("y", "z"), None, None)

    return jax.shard_map(
        shards,
        mesh=split,
        in_specs=(rows, rows, rows, P(), P(), P(), P(), P(), P(), P(), P(), P("img", None)),
        out_specs=rows,
        check_vma=False,
    )
```

```python
import functools

import jax
import jax.numpy as jnp
import numpy as np
from jax import lax
from jax.experimental import pallas as pl
from jax.experimental.pallas import tpu as pltpu
from jax.sharding import Mesh
from jax.sharding import PartitionSpec as P

GROUPS = 32
HEAD_DIM = 64
EPSILON = 1e-05
LANES = 128
PIECES = 8


F32 = jnp.float32
BF16 = jnp.bfloat16
VMEM = pl.BlockSpec(memory_space=pltpu.VMEM)


def normalize(values, gain, bias):
    values = values.astype(F32)
    centre = jnp.mean(values, -1, keepdims=True)
    centred = values - centre
    spread = jnp.mean(centred * centred, -1, keepdims=True)
    return (centred * lax.rsqrt(spread + EPSILON) * gain + bias).astype(BF16)


def as_row(ref):
    return ref[...].reshape(1, -1)


def stale_norm_kernel(x_ref, gain_ref, bias_ref, all_ref, *out_refs):
    normed = normalize(x_ref[...], as_row(gain_ref), as_row(bias_ref))
    all_ref[...] = normed
    rows = out_refs[0].shape[0]
    for index, out_ref in enumerate(out_refs):
        out_ref[...] = normed[index * rows : (index + 1) * rows]


def query_kernel(x_ref, gain_ref, bias_ref, w_ref, q_ref, normed_ref):
    normed = normalize(x_ref[...], as_row(gain_ref), as_row(bias_ref))
    normed_ref[...] = normed
    projected = jnp.dot(normed, w_ref[...], preferred_element_type=F32).astype(BF16)
    q_ref[...] = (projected.astype(F32) * HEAD_DIM ** (-0.5)).astype(BF16)


def scores_of(queries, keys):
    return lax.dot_general(
        queries, keys, (((1,), (1,)), ((), ())), preferred_element_type=F32
    )


def project(x, wk_ref, wv_ref, kv_scr, slot):
    weights = jnp.concatenate([wk_ref[...], wv_ref[...]], axis=1)
    kv_scr[slot] = jnp.dot(x, weights, preferred_element_type=F32).astype(BF16)


def attend_kernel(
    q0_ref, q1_ref, q2_ref, q3_ref,
    z1_ref, z2_ref, z3_ref, fresh_ref, own_ref,
    wk0_ref, wv0_ref, wk_ref, wv_ref,
    o0_ref, o1_ref, o2_ref, o3_ref,
    x_scr, kv_scr, tile_scr,
    *, sample,
):
    pair = pl.program_id(0)
    rows = z2_ref.shape[0]
    channels = fresh_ref.shape[1]
    part = slice(sample * rows, (sample + 1) * rows)
    out_refs = (o0_ref, o1_ref, o2_ref, o3_ref)

    @pl.when(pair == 0)
    def _():
        for index, ref in enumerate((z1_ref, z2_ref, z3_ref, fresh_ref, own_ref)):
            x_scr[index * rows : (index + 1) * rows, :] = ref[...] if index == 1 else ref[part, :]
        tile_scr[...] = jnp.zeros_like(tile_scr)
        project(x_scr[...], wk0_ref, wv0_ref, kv_scr, 0)

    current = pair & 1
    keys, values = kv_scr[current, :, :LANES], kv_scr[current, :, LANES:]
    low_all = lax.broadcasted_iota(jnp.int32, keys.shape, 1) < HEAD_DIM
    zero = jnp.zeros((), BF16)
    one = jnp.ones((), BF16)
    low_values = jnp.concatenate(
        [jnp.where(low_all, values, zero), jnp.where(low_all, one, zero)], axis=1
    )
    high_values = jnp.concatenate(
        [jnp.where(low_all, zero, values), jnp.where(low_all, zero, one)], axis=1
    )
    common, fresh, own = slice(0, 3 * rows), slice(3 * rows, 4 * rows), slice(4 * rows, 5 * rows)
    lanes = pl.ds(pl.multiple_of(pair * LANES, LANES), LANES)
    mine = q0_ref[part, lanes]
    others = jnp.concatenate([ref[part, lanes] for ref in (q1_ref, q2_ref, q3_ref)], 0)

    def halves(x):
        low_part = lax.broadcasted_iota(jnp.int32, x.shape, 1) < HEAD_DIM
        return jnp.concatenate([jnp.where(low_part, x, zero), jnp.where(low_part, zero, x)], 0)

    mine, others = halves(mine), halves(others)
    shared = scores_of(jnp.concatenate([mine, others], 0), keys[common])
    single = jnp.concatenate([scores_of(mine, keys[fresh]), scores_of(others, keys[own])], 0)
    top = single
    for index in range(3):
        top = jnp.maximum(top, shared[:, index * LANES : (index + 1) * LANES])
    top = jnp.max(top, -1, keepdims=True)
    shared = jnp.exp(shared - top).astype(BF16)
    single = jnp.exp(single - top).astype(BF16)

    def paired(x):
        return (
            jnp.concatenate([x[:rows], x[2 * rows : 5 * rows]], 0),
            jnp.concatenate([x[rows : 2 * rows], x[5 * rows :]], 0),
        )

    summed = jnp.dot(
        jnp.concatenate(paired(shared), 1),
        jnp.concatenate([low_values[common], high_values[common]], 0),
        preferred_element_type=F32,
    )
    single = jnp.concatenate(paired(single), 1)
    summed = summed + jnp.concatenate(
        [
            jnp.dot(
                single[:rows],
                jnp.concatenate([low_values[fresh], high_values[fresh]], 0),
                preferred_element_type=F32,
            ),
            jnp.dot(
                single[rows:],
                jnp.concatenate([low_values[own], high_values[own]], 0),
                preferred_element_type=F32,
            ),
        ],
        0,
    )
    total = summed[:, LANES:]
    mixed = (summed[:, :LANES] / total).astype(BF16)
    for index, o_ref in enumerate(out_refs):
        o_ref[:, lanes] = mixed[index * rows : (index + 1) * rows]
    lane = lax.broadcasted_iota(jnp.int32, total.shape, 1)
    low_top, high_top = paired(top)
    rest = jnp.where(lane < HEAD_DIM, low_top, high_top) + jnp.log(total)
    slot = lane & (HEAD_DIM - 1)
    tile = tile_scr[...]
    for piece in range(3):
        rounded = rest.astype(BF16).astype(F32)
        tile = jnp.where(slot == pair + piece * PIECES, rounded, tile)
        rest = rest - rounded
    tile_scr[...] = tile
    project(x_scr[...], wk_ref, wv_ref, kv_scr, 1 - current)

    @pl.when(pair == pl.num_programs(0) - 1)
    def _():
        for index, o_ref in enumerate(out_refs):
            o_ref[:, channels:] = tile_scr[index * rows : (index + 1) * rows, :].astype(BF16)


def spread_matrix(channels):
    out = np.zeros((LANES, channels), np.float32)
    for channel in range(channels):
        head = channel // HEAD_DIM
        base = (head % 2) * HEAD_DIM + head // 2
        for piece in range(3):
            out[base + piece * PIECES, channel] = 1
    return out


def exact_dot(x, ones):
    total = None
    for _ in range(3):
        rounded = x.astype(BF16)
        part = jnp.dot(rounded, ones, preferred_element_type=F32)
        total = part if total is None else total + part
        x = x - rounded.astype(F32)
    return total


def merge_kernel(
    o0_ref, o1_ref, o2_ref, o3_ref, hidden_ref, w_ref, spread_ref, gather_ref, *rest_refs, sample
):
    channels = hidden_ref.shape[1]
    rows = hidden_ref.shape[0]
    refs = (o0_ref, o1_ref, o2_ref, o3_ref)
    tiles = jnp.concatenate([ref[:, channels:] for ref in refs], 0)
    logs = jnp.dot(tiles, spread_ref[...], preferred_element_type=F32)
    logs = [logs[index * rows : (index + 1) * rows] for index in range(4)]
    top = jnp.maximum(jnp.maximum(logs[0], logs[1]), jnp.maximum(logs[2], logs[3]))
    numer = denom = None
    for ref, one in zip(refs, logs):
        factor = jnp.exp(one - top)
        upper = factor * ref[:, :channels].astype(F32)
        numer, denom = (upper, factor) if numer is None else (numer + upper, denom + factor)
    attended = (numer / denom).astype(BF16)
    residual = (
        hidden_ref[...].astype(F32) + jnp.dot(attended, w_ref[...], preferred_element_type=F32)
    ).astype(BF16)
    res_ref, stat_ref = rest_refs[-2:]
    res_ref[...] = residual
    wide = residual.astype(F32)
    sums = jnp.concatenate(
        [jnp.sum(wide, 0, keepdims=True), jnp.sum(wide * wide, 0, keepdims=True)]
        + [jnp.zeros((6, channels), F32)],
        0,
    )
    sums = exact_dot(sums, gather_ref[...])
    if sample:
        sums = pltpu.roll(sums, 2 * sample, 0) + rest_refs[0][...]
        stat_ref[...] = jnp.broadcast_to(sums[None], stat_ref.shape)
    else:
        stat_ref[...] = sums


def shifted(x, by, cols):
    rolled = pltpu.roll(x, by % x.shape[0], 0)
    col = lax.broadcasted_iota(jnp.int32, x.shape, 0) & (cols - 1)
    edge = 0 if by == 1 else cols - 1
    return jnp.where(col == edge, 0.0, rolled).astype(BF16)


def taps(x, weights, cols):
    wide = x.astype(F32)
    unfolded = jnp.concatenate([shifted(wide, 1, cols), x, shifted(wide, -1, cols)], 1)
    weights = weights.reshape(-1, weights.shape[-1])
    return jnp.dot(unfolded, weights, preferred_element_type=F32)


def rim_kernel(above_ref, below_ref, w_ref, bias_ref, shift_ref, out_ref, *, cols):
    total = taps(above_ref[...], w_ref[0], cols) + taps(below_ref[...], w_ref[2], cols)
    total += as_row(bias_ref)
    for sample in range(total.shape[0] // cols):
        part = slice(sample * cols, (sample + 1) * cols)
        out_ref[part, :] = total[part] + shift_ref[sample : sample + 1, :]


def final_kernel(
    res0_ref, res1_ref, stat_ref, gain_ref, bias_ref, scatter_ref, w_ref, rim_ref, out_ref,
    *, cols, cells
):
    activated = []
    wide = []
    sums = exact_dot(jnp.sum(stat_ref[...], 0), scatter_ref[...])
    gain, bias = as_row(gain_ref), as_row(bias_ref)
    for sample, res_ref in enumerate((res0_ref, res1_ref)):
        mean = sums[2 * sample : 2 * sample + 1] / cells
        var = sums[2 * sample + 1 : 2 * sample + 2] / cells - mean * mean
        residual = res_ref[...].astype(F32)
        wide.append(residual)
        normalized = (residual - mean) * lax.rsqrt(var + EPSILON)
        value = normalized * gain + bias
        activated.append((value / (1.0 + jnp.exp(-value))).astype(BF16))
    x = jnp.concatenate(activated, 0)
    out_ref[...] = (
        taps(x, w_ref[1], cols) + rim_ref[...] + jnp.concatenate(wide, 0)
    ).astype(BF16)


def ring(by, count):
    return [(i, (i + by) % count) for i in range(count)]


def call(kernel, out_shape, *args, flops=1000000, chip=(), slow=(), **kwargs):
    spaces = {**dict.fromkeys(chip, pltpu.VMEM), **dict.fromkeys(slow, pltpu.HBM)}
    args = [
        pltpu.with_memory_space_constraint(x, spaces[index]) if index in spaces else x
        for index, x in enumerate(args)
    ]
    return pl.pallas_call(
        kernel,
        out_shape=out_shape,
        compiler_params=pltpu.CompilerParams(vmem_limit_bytes=24 * 2 ** 20),
        cost_estimate=pl.CostEstimate(flops=flops, bytes_accessed=1000000, transcendentals=0),
        **kwargs,
    )(*args)


def shards(
    hidden, stale_attn_in, stale_conv_in, ln_gain, ln_bias, w_qkv, w_out,
    gn_gain, gn_bias, conv_weight, conv_bias, time_shift,
):
    samples, rows_dev, cols, channels = hidden.shape
    tokens = rows_dev * cols
    every = samples * tokens
    pair_count = channels // LANES
    y_count, z_count = lax.axis_size("y"), lax.axis_size("z")
    count = y_count * z_count
    hid = hidden.reshape(every, channels)
    block = pltpu.VMEM((tokens, channels), BF16)
    full = pl.BlockSpec((every, channels), lambda i: (0, 0))
    vector = pl.BlockSpec((channels,), lambda i: (0,))
    shifts = (1, 3, 2)

    both = pltpu.VMEM((every, channels), BF16)
    stale, *parts = call(
        stale_norm_kernel, [both] + [block] * samples,
        stale_attn_in.reshape(every, channels), ln_gain, ln_bias,
        grid=(1,),
        in_specs=[full, vector, vector],
        out_specs=[VMEM] * (1 + samples),
        slow=(0, 1, 2),
        flops=6 * 10 ** 9,
    )
    beside = [lax.ppermute(stale, "z", ring(by, z_count)) for by in (1, 3)]
    across = [lax.ppermute(one, "z", ring(2, z_count)) for one in parts]
    queries, fresh = call(
        query_kernel, [both] * 2, hid, ln_gain, ln_bias, w_qkv,
        grid=(1,),
        in_specs=[VMEM, VMEM, VMEM, pl.BlockSpec((channels, channels), lambda i: (0, 0))],
        out_specs=[VMEM] * 2,
        flops=6 * 10 ** 9,
    )
    all_queries = [queries] + [lax.ppermute(queries, "y", ring(by, y_count)) for by in shifts]
    conv_rows = stale_conv_in.reshape(every, channels)
    above = lax.ppermute(conv_rows, ("y", "z"), [(i, i + 1) for i in range(count - 1)])
    below = lax.ppermute(conv_rows, ("y", "z"), [(i + 1, i) for i in range(count - 1)])

    wide = channels + LANES
    spread = jnp.asarray(spread_matrix(channels), BF16)
    group = np.arange(channels) // (channels // GROUPS)
    gather = group[:, None] == np.arange(LANES)[None, :]
    ext = pltpu.VMEM((tokens, wide), BF16)
    back = []
    for s in range(samples):
        outs = call(
            functools.partial(attend_kernel, sample=s), [ext] * 4,
            *all_queries, beside[0], across[s], beside[1], fresh, stale,
            w_qkv, w_qkv, w_qkv, w_qkv,
            grid=(pair_count,),
            in_specs=[VMEM] * 9
            + [
                pl.BlockSpec((channels, LANES), lambda p: (0, pair_count)),
                pl.BlockSpec((channels, LANES), lambda p: (0, 2 * pair_count)),
                pl.BlockSpec((channels, LANES), lambda p: (0, jnp.minimum(pair_count + p + 1, 2 * pair_count - 1))),
                pl.BlockSpec((channels, LANES), lambda p: (0, jnp.minimum(2 * pair_count + p + 1, 3 * pair_count - 1))),
            ],
            out_specs=[VMEM] * 4,
            scratch_shapes=[
                pltpu.VMEM((5 * tokens, channels), BF16),
                pltpu.VMEM((2, 5 * tokens, 2 * LANES), BF16),
                pltpu.VMEM((4 * tokens, LANES), F32),
            ],
            flops=6 * 10 ** 9,
            chip=range(9),
        )
        back.append(
            [outs[0]]
            + [lax.ppermute(one, "y", ring(-by, y_count)) for one, by in zip(outs[1:], shifts)]
        )
    rim = call(
        functools.partial(rim_kernel, cols=cols),
        pltpu.VMEM((every, channels), F32),
        above, below, conv_weight, conv_bias, time_shift,
        in_specs=[VMEM] * 5,
        out_specs=VMEM,
        flops=12 * every * channels * channels,
        chip=(0, 1, 2),
    )
    residuals, stats = [], []
    for s in range(samples):
        small = pltpu.VMEM((8, LANES), F32)
        if s:
            small = pltpu.VMEM((count, 8, LANES), F32)
        res, stat = call(
            functools.partial(merge_kernel, sample=s), [block, small],
            *back[s], hid, w_out, spread, jnp.asarray(gather, BF16), *stats,
            grid=(1,),
            in_specs=[VMEM] * 4
            + [pl.BlockSpec((tokens, channels), lambda i, s=s: (s, 0))]
            + [VMEM] * (3 + len(stats)),
            out_specs=[VMEM, VMEM],
            flops=10 ** 9,
            chip=(0, 1, 2, 3, 5) + (8,) * s,
        )
        residuals.append(res)
        stats = [stat]
    shared = lax.all_to_all(stats[0], ("y", "z"), 0, 0)
    out = call(
        functools.partial(
            final_kernel, cols=cols, cells=float(count * tokens * (channels // GROUPS))
        ),
        jax.ShapeDtypeStruct((every, channels), BF16),
        *residuals, shared, gn_gain, gn_bias, jnp.asarray(gather.T, BF16), conv_weight, rim,
        in_specs=[VMEM] * 8,
        out_specs=VMEM,
        chip=(0, 1, 2, 6, 7),
        flops=6 * every * channels * channels,
    )
    return out.reshape(hidden.shape)


def solution(mesh):
    split = Mesh(mesh.devices.reshape(mesh.shape["img"], 4, 4), ("img", "y", "z"))
    rows = P("img", ("y", "z"), None, None)

    return jax.shard_map(
        shards,
        mesh=split,
        in_specs=(rows, rows, rows, P(), P(), P(), P(), P(), P(), P(), P(), P("img", None)),
        out_specs=rows,
        check_vma=False,
    )
```

```python
import functools

import jax
import jax.numpy as jnp
import numpy as np
from jax import lax
from jax.experimental import pallas as pl
from jax.experimental.pallas import tpu as pltpu
from jax.sharding import Mesh
from jax.sharding import PartitionSpec as P

GROUPS = 32
HEAD_DIM = 64
EPSILON = 1e-05
LANES = 128
PIECES = 8


F32 = jnp.float32
BF16 = jnp.bfloat16
VMEM = pl.BlockSpec(memory_space=pltpu.VMEM)


def normalize(values, gain, bias):
    values = values.astype(F32)
    centre = jnp.mean(values, -1, keepdims=True)
    centred = values - centre
    spread = jnp.mean(centred * centred, -1, keepdims=True)
    return (centred * lax.rsqrt(spread + EPSILON) * gain + bias).astype(BF16)


def as_row(ref):
    return ref[...].reshape(1, -1)


def stale_norm_kernel(x_ref, gain_ref, bias_ref, *out_refs):
    normed = normalize(x_ref[...], as_row(gain_ref), as_row(bias_ref))
    rows = out_refs[0].shape[0]
    for index, out_ref in enumerate(out_refs):
        out_ref[...] = normed[index * rows : (index + 1) * rows]


def query_kernel(x_ref, gain_ref, bias_ref, w_ref, q_ref, normed_ref):
    normed = normalize(x_ref[...], as_row(gain_ref), as_row(bias_ref))
    normed_ref[...] = normed
    projected = jnp.dot(normed, w_ref[...], preferred_element_type=F32).astype(BF16)
    q_ref[...] = (projected.astype(F32) * HEAD_DIM ** (-0.5)).astype(BF16)


def scores_of(queries, keys):
    return lax.dot_general(
        queries, keys, (((1,), (1,)), ((), ())), preferred_element_type=F32
    )


def project(x, wk_ref, wv_ref, kv_scr, slot):
    weights = jnp.concatenate([wk_ref[...], wv_ref[...]], axis=1)
    kv_scr[slot] = jnp.dot(x, weights, preferred_element_type=F32).astype(BF16)


def attend_kernel(
    q0_ref, q1_ref, q2_ref, q3_ref,
    z1_ref, z2_ref, z3_ref, fresh_ref, own_ref,
    wk0_ref, wv0_ref, wk_ref, wv_ref, conv_ref,
    o0_ref, o1_ref, o2_ref, o3_ref,
    *refs, sample,
):
    x_scr, kv_scr, tile_scr = refs[-4:-1]
    pair = pl.program_id(0)
    fetch = pltpu.make_async_copy(conv_ref, refs[0], refs[-1]) if len(refs) > 4 else None
    rows = z2_ref.shape[0]
    channels = fresh_ref.shape[1]
    part = slice(sample * rows, (sample + 1) * rows)
    out_refs = (o0_ref, o1_ref, o2_ref, o3_ref)

    @pl.when(pair == 0)
    def _():
        if fetch:
            fetch.start()
        for index, ref in enumerate((z1_ref, z2_ref, z3_ref, fresh_ref, own_ref)):
            x_scr[index * rows : (index + 1) * rows, :] = ref[part, :] if index == 3 else ref[...]
        tile_scr[...] = jnp.zeros_like(tile_scr)
        project(x_scr[...], wk0_ref, wv0_ref, kv_scr, 0)

    current = pair & 1
    keys, values = kv_scr[current, :, :LANES], kv_scr[current, :, LANES:]
    low_all = lax.broadcasted_iota(jnp.int32, keys.shape, 1) < HEAD_DIM
    zero = jnp.zeros((), BF16)
    one = jnp.ones((), BF16)
    low_values = jnp.concatenate(
        [jnp.where(low_all, values, zero), jnp.where(low_all, one, zero)], axis=1
    )
    high_values = jnp.concatenate(
        [jnp.where(low_all, zero, values), jnp.where(low_all, zero, one)], axis=1
    )
    common, fresh, own = slice(0, 3 * rows), slice(3 * rows, 4 * rows), slice(4 * rows, 5 * rows)
    lanes = pl.ds(pl.multiple_of(pair * LANES, LANES), LANES)
    mine = q0_ref[part, lanes]
    others = jnp.concatenate([ref[part, lanes] for ref in (q1_ref, q2_ref, q3_ref)], 0)

    def halves(x):
        low_part = lax.broadcasted_iota(jnp.int32, x.shape, 1) < HEAD_DIM
        return jnp.concatenate([jnp.where(low_part, x, zero), jnp.where(low_part, zero, x)], 0)

    mine, others = halves(mine), halves(others)
    shared = scores_of(jnp.concatenate([mine, others], 0), keys[common])
    single = jnp.concatenate([scores_of(mine, keys[fresh]), scores_of(others, keys[own])], 0)
    top = single
    for index in range(3):
        top = jnp.maximum(top, shared[:, index * LANES : (index + 1) * LANES])
    top = jnp.max(top, -1, keepdims=True)
    shared = jnp.exp(shared - top).astype(BF16)
    single = jnp.exp(single - top).astype(BF16)

    def paired(x):
        return (
            jnp.concatenate([x[:rows], x[2 * rows : 5 * rows]], 0),
            jnp.concatenate([x[rows : 2 * rows], x[5 * rows :]], 0),
        )

    summed = jnp.dot(
        jnp.concatenate(paired(shared), 1),
        jnp.concatenate([low_values[common], high_values[common]], 0),
        preferred_element_type=F32,
    )
    single = jnp.concatenate(paired(single), 1)
    summed = summed + jnp.concatenate(
        [
            jnp.dot(
                single[:rows],
                jnp.concatenate([low_values[fresh], high_values[fresh]], 0),
                preferred_element_type=F32,
            ),
            jnp.dot(
                single[rows:],
                jnp.concatenate([low_values[own], high_values[own]], 0),
                preferred_element_type=F32,
            ),
        ],
        0,
    )
    total = summed[:, LANES:]
    mixed = (summed[:, :LANES] / total).astype(BF16)
    for index, o_ref in enumerate(out_refs):
        o_ref[:, lanes] = mixed[index * rows : (index + 1) * rows]
    lane = lax.broadcasted_iota(jnp.int32, total.shape, 1)
    low_top, high_top = paired(top)
    rest = jnp.where(lane < HEAD_DIM, low_top, high_top) + jnp.log(total)
    slot = lane & (HEAD_DIM - 1)
    tile = tile_scr[...]
    for piece in range(3):
        rounded = rest.astype(BF16).astype(F32)
        tile = jnp.where(slot == pair + piece * PIECES, rounded, tile)
        rest = rest - rounded
    tile_scr[...] = tile
    project(x_scr[...], wk_ref, wv_ref, kv_scr, 1 - current)

    @pl.when(pair == pl.num_programs(0) - 1)
    def _():
        if fetch:
            fetch.wait()
        for index, o_ref in enumerate(out_refs):
            o_ref[:, channels:] = tile_scr[index * rows : (index + 1) * rows, :].astype(BF16)


def spread_matrix(channels):
    out = np.zeros((LANES, channels), np.float32)
    for channel in range(channels):
        head = channel // HEAD_DIM
        base = (head % 2) * HEAD_DIM + head // 2
        for piece in range(3):
            out[base + piece * PIECES, channel] = 1
    return out


def exact_dot(x, ones):
    total = None
    for _ in range(3):
        rounded = x.astype(BF16)
        part = jnp.dot(rounded, ones, preferred_element_type=F32)
        total = part if total is None else total + part
        x = x - rounded.astype(F32)
    return total


def merge_kernel(
    o0_ref, o1_ref, o2_ref, o3_ref, hidden_ref, w_ref, spread_ref, gather_ref, *rest_refs, sample
):
    channels = hidden_ref.shape[1]
    rows = hidden_ref.shape[0]
    refs = (o0_ref, o1_ref, o2_ref, o3_ref)
    tiles = jnp.concatenate([ref[:, channels:] for ref in refs], 0)
    logs = jnp.dot(tiles, spread_ref[...], preferred_element_type=F32)
    logs = [logs[index * rows : (index + 1) * rows] for index in range(4)]
    top = jnp.maximum(jnp.maximum(logs[0], logs[1]), jnp.maximum(logs[2], logs[3]))
    numer = denom = None
    for ref, one in zip(refs, logs):
        factor = jnp.exp(one - top)
        upper = factor * ref[:, :channels].astype(F32)
        numer, denom = (upper, factor) if numer is None else (numer + upper, denom + factor)
    attended = (numer / denom).astype(BF16)
    residual = (
        hidden_ref[...].astype(F32) + jnp.dot(attended, w_ref[...], preferred_element_type=F32)
    ).astype(BF16)
    res_ref, stat_ref = rest_refs[-2:]
    res_ref[...] = residual
    wide = residual.astype(F32)
    sums = jnp.concatenate(
        [jnp.sum(wide, 0, keepdims=True), jnp.sum(wide * wide, 0, keepdims=True)]
        + [jnp.zeros((6, channels), F32)],
        0,
    )
    sums = exact_dot(sums, gather_ref[...])
    if sample:
        sums = pltpu.roll(sums, 2 * sample, 0) + rest_refs[0][...]
    stat_ref[...] = sums


def shifted(x, by, cols):
    rolled = pltpu.roll(x, by % x.shape[0], 0)
    col = lax.broadcasted_iota(jnp.int32, x.shape, 0) & (cols - 1)
    edge = 0 if by == 1 else cols - 1
    return jnp.where(col == edge, 0.0, rolled).astype(BF16)


def taps(x, weights, cols):
    wide = x.astype(F32)
    unfolded = jnp.concatenate([shifted(wide, 1, cols), x, shifted(wide, -1, cols)], 1)
    weights = weights.reshape(-1, weights.shape[-1])
    return jnp.dot(unfolded, weights, preferred_element_type=F32)


def rim_kernel(above_ref, below_ref, w_ref, bias_ref, shift_ref, out_ref, *, cols):
    total = taps(above_ref[...], w_ref[0], cols) + taps(below_ref[...], w_ref[2], cols)
    total += as_row(bias_ref)
    for sample in range(total.shape[0] // cols):
        part = slice(sample * cols, (sample + 1) * cols)
        out_ref[part, :] = total[part] + shift_ref[sample : sample + 1, :]


def add_kernel(*refs):
    refs[-1][...] = (refs[0][...] + refs[1][...]) + (refs[2][...] + refs[3][...])


def final_kernel(
    res0_ref, res1_ref, s0_ref, s1_ref, s2_ref, s3_ref, gain_ref, bias_ref, scatter_ref, w_ref, rim_ref, out_ref,
    *, cols, cells
):
    activated = []
    wide = []
    sums = (s0_ref[...] + s1_ref[...]) + (s2_ref[...] + s3_ref[...])
    sums = exact_dot(sums, scatter_ref[...])
    gain, bias = as_row(gain_ref), as_row(bias_ref)
    for sample, res_ref in enumerate((res0_ref, res1_ref)):
        mean = sums[2 * sample : 2 * sample + 1] / cells
        var = sums[2 * sample + 1 : 2 * sample + 2] / cells - mean * mean
        residual = res_ref[...].astype(F32)
        wide.append(residual)
        normalized = (residual - mean) * lax.rsqrt(var + EPSILON)
        value = normalized * gain + bias
        activated.append((value / (1.0 + jnp.exp(-value))).astype(BF16))
    x = jnp.concatenate(activated, 0)
    out_ref[...] = (
        taps(x, w_ref[1], cols) + rim_ref[...] + jnp.concatenate(wide, 0)
    ).astype(BF16)


def ring(by, count):
    return [(i, (i + by) % count) for i in range(count)]


def call(kernel, out_shape, *args, flops=1000000, chip=(), slow=(), **kwargs):
    spaces = {**dict.fromkeys(chip, pltpu.VMEM), **dict.fromkeys(slow, pltpu.HBM)}
    args = [
        pltpu.with_memory_space_constraint(x, spaces[index]) if index in spaces else x
        for index, x in enumerate(args)
    ]
    return pl.pallas_call(
        kernel,
        out_shape=out_shape,
        compiler_params=pltpu.CompilerParams(vmem_limit_bytes=24 * 2 ** 20),
        cost_estimate=pl.CostEstimate(flops=flops, bytes_accessed=1000000, transcendentals=0),
        **kwargs,
    )(*args)


def shards(
    hidden, stale_attn_in, stale_conv_in, ln_gain, ln_bias, w_qkv, w_out,
    gn_gain, gn_bias, conv_weight, conv_bias, time_shift,
):
    samples, rows_dev, cols, channels = hidden.shape
    tokens = rows_dev * cols
    every = samples * tokens
    pair_count = channels // LANES
    y_count, z_count = lax.axis_size("y"), lax.axis_size("z")
    count = y_count * z_count
    hid = hidden.reshape(every, channels)
    block = pltpu.VMEM((tokens, channels), BF16)
    full = pl.BlockSpec((every, channels), lambda i: (0, 0))
    vector = pl.BlockSpec((channels,), lambda i: (0,))
    shifts = (1, 3, 2)

    both = pltpu.VMEM((every, channels), BF16)
    stale = call(
        stale_norm_kernel, [block] * samples,
        stale_attn_in.reshape(every, channels), ln_gain, ln_bias,
        grid=(1,),
        in_specs=[full, vector, vector],
        out_specs=[VMEM] * samples,
        slow=(0, 1, 2),
        flops=6 * 10 ** 9,
    )
    along = [[lax.ppermute(one, "z", ring(by, z_count)) for by in (1, 2, 3)] for one in stale]
    queries, fresh = call(
        query_kernel, [both] * 2, hid, ln_gain, ln_bias, w_qkv,
        grid=(1,),
        in_specs=[VMEM, VMEM, VMEM, pl.BlockSpec((channels, channels), lambda i: (0, 0))],
        out_specs=[VMEM] * 2,
        flops=6 * 10 ** 9,
    )
    all_queries = [queries] + [lax.ppermute(queries, "y", ring(by, y_count)) for by in shifts]
    conv_rows = stale_conv_in.reshape(every, channels)
    above = lax.ppermute(conv_rows, ("y", "z"), [(i, i + 1) for i in range(count - 1)])
    below = lax.ppermute(conv_rows, ("y", "z"), [(i + 1, i) for i in range(count - 1)])

    wide = channels + LANES
    spread = jnp.asarray(spread_matrix(channels), BF16)
    group = np.arange(channels) // (channels // GROUPS)
    gather = group[:, None] == np.arange(LANES)[None, :]
    ext = pltpu.VMEM((tokens, wide), BF16)
    back = []
    for s in range(samples):
        extra = [pltpu.VMEM(conv_weight.shape, BF16)] * (s == samples - 1)
        outs = call(
            functools.partial(attend_kernel, sample=s), [ext] * 4 + extra,
            *all_queries, *along[s], fresh, stale[s],
            w_qkv, w_qkv, w_qkv, w_qkv, conv_weight,
            grid=(pair_count,),
            in_specs=[VMEM] * 9
            + [
                pl.BlockSpec((channels, LANES), lambda p: (0, pair_count)),
                pl.BlockSpec((channels, LANES), lambda p: (0, 2 * pair_count)),
                pl.BlockSpec((channels, LANES), lambda p: (0, jnp.minimum(pair_count + p + 1, 2 * pair_count - 1))),
                pl.BlockSpec((channels, LANES), lambda p: (0, jnp.minimum(2 * pair_count + p + 1, 3 * pair_count - 1))),
                pl.BlockSpec(memory_space=pl.ANY),
            ],
            out_specs=[VMEM] * (4 + len(extra)),
            scratch_shapes=[
                pltpu.VMEM((5 * tokens, channels), BF16),
                pltpu.VMEM((2, 5 * tokens, 2 * LANES), BF16),
                pltpu.VMEM((4 * tokens, LANES), F32),
                pltpu.SemaphoreType.DMA,
            ],
            flops=6 * 10 ** 9,
            chip=range(9),
            slow=(13,),
        )
        back.append(
            [outs[0]]
            + [lax.ppermute(one, "y", ring(-by, y_count)) for one, by in zip(outs[1:4], shifts)]
        )
    conv_on_chip = outs[4]
    rim = call(
        functools.partial(rim_kernel, cols=cols),
        pltpu.VMEM((every, channels), F32),
        above, below, conv_on_chip, conv_bias, time_shift,
        in_specs=[VMEM] * 5,
        out_specs=VMEM,
        flops=12 * every * channels * channels,
        chip=(0, 1, 2),
    )
    residuals, stats = [], []
    for s in range(samples):
        small = pltpu.VMEM((8, LANES), F32)
        res, stat = call(
            functools.partial(merge_kernel, sample=s), [block, small],
            *back[s], hid, w_out, spread, jnp.asarray(gather, BF16), *stats,
            grid=(1,),
            in_specs=[VMEM] * 4
            + [pl.BlockSpec((tokens, channels), lambda i, s=s: (s, 0))]
            + [VMEM] * (3 + len(stats)),
            out_specs=[VMEM, VMEM],
            flops=6 * 10 ** 9,
            chip=(0, 1, 2, 3, 5) + (8,) * s,
        )
        residuals.append(res)
        stats = [stat]
    stat = stats[0]
    along_y = [stat] + [lax.ppermute(stat, "y", ring(by, y_count)) for by in shifts]
    stat = call(add_kernel, small, *along_y, in_specs=[VMEM] * 4, out_specs=VMEM, chip=range(4))
    along_z = [stat] + [lax.ppermute(stat, "z", ring(by, z_count)) for by in shifts]
    out = call(
        functools.partial(
            final_kernel, cols=cols, cells=float(count * tokens * (channels // GROUPS))
        ),
        jax.ShapeDtypeStruct((every, channels), BF16),
        *residuals, *along_z, gn_gain, gn_bias, jnp.asarray(gather.T, BF16), conv_on_chip, rim,
        in_specs=[VMEM] * 11,
        out_specs=VMEM,
        chip=(0, 1, 2, 3, 4, 5, 9, 10),
        flops=6 * every * channels * channels,
    )
    return out.reshape(hidden.shape)


def solution(mesh):
    split = Mesh(mesh.devices.reshape(mesh.shape["img"], 4, 4), ("img", "y", "z"))
    rows = P("img", ("y", "z"), None, None)

    return jax.shard_map(
        shards,
        mesh=split,
        in_specs=(rows, rows, rows, P(), P(), P(), P(), P(), P(), P(), P(), P("img", None)),
        out_specs=rows,
        check_vma=False,
    )
```

```python
import functools

import jax
import jax.numpy as jnp
import numpy as np
from jax import lax
from jax.experimental import pallas as pl
from jax.experimental.pallas import tpu as pltpu
from jax.sharding import Mesh
from jax.sharding import PartitionSpec as P

GROUPS = 32
HEAD_DIM = 64
EPSILON = 1e-05
LANES = 128
PIECES = 8


F32 = jnp.float32
BF16 = jnp.bfloat16
VMEM = pl.BlockSpec(memory_space=pltpu.VMEM)


def normalize(values, gain, bias):
    values = values.astype(F32)
    centre = jnp.mean(values, -1, keepdims=True)
    centred = values - centre
    spread = jnp.mean(centred * centred, -1, keepdims=True)
    return (centred * lax.rsqrt(spread + EPSILON) * gain + bias).astype(BF16)


def as_row(ref):
    return ref[...].reshape(1, -1)


def stale_norm_kernel(x_ref, gain_ref, bias_ref, *out_refs):
    normed = normalize(x_ref[...], as_row(gain_ref), as_row(bias_ref))
    rows = out_refs[0].shape[0]
    for index, out_ref in enumerate(out_refs):
        out_ref[...] = normed[index * rows : (index + 1) * rows]


def query_kernel(x_ref, gain_ref, bias_ref, w_ref, q_ref, normed_ref):
    normed = normalize(x_ref[...], as_row(gain_ref), as_row(bias_ref))
    normed_ref[...] = normed
    projected = jnp.dot(normed, w_ref[...], preferred_element_type=F32).astype(BF16)
    q_ref[...] = (projected.astype(F32) * HEAD_DIM ** (-0.5)).astype(BF16)


def scores_of(queries, keys):
    return lax.dot_general(
        queries, keys, (((1,), (1,)), ((), ())), preferred_element_type=F32
    )


def project(x, wk_ref, wv_ref, kv_scr, slot):
    weights = jnp.concatenate([wk_ref[...], wv_ref[...]], axis=1)
    kv_scr[slot] = jnp.dot(x, weights, preferred_element_type=F32).astype(BF16)


def attend_kernel(
    q0_ref, q1_ref, q2_ref, q3_ref,
    z1_ref, z2_ref, z3_ref, fresh_ref, own_ref,
    wk0_ref, wv0_ref, wk_ref, wv_ref, conv_ref,
    o0_ref, o1_ref, o2_ref, o3_ref,
    *refs, sample,
):
    x_scr, kv_scr, tile_scr = refs[-4:-1]
    pair = pl.program_id(0)
    fetch = pltpu.make_async_copy(conv_ref, refs[0], refs[-1]) if len(refs) > 4 else None
    rows = z2_ref.shape[0]
    channels = fresh_ref.shape[1]
    part = slice(sample * rows, (sample + 1) * rows)
    out_refs = (o0_ref, o1_ref, o2_ref, o3_ref)

    @pl.when(pair == 0)
    def _():
        if fetch:
            fetch.start()
        for index, ref in enumerate((z1_ref, z2_ref, z3_ref, fresh_ref, own_ref)):
            x_scr[index * rows : (index + 1) * rows, :] = ref[part, :] if index == 3 else ref[...]
        tile_scr[...] = jnp.zeros_like(tile_scr)
        project(x_scr[...], wk0_ref, wv0_ref, kv_scr, 0)

    current = pair & 1
    keys, values = kv_scr[current, :, :LANES], kv_scr[current, :, LANES:]
    low_all = lax.broadcasted_iota(jnp.int32, keys.shape, 1) < HEAD_DIM
    zero = jnp.zeros((), BF16)
    one = jnp.ones((), BF16)
    low_values = jnp.concatenate(
        [jnp.where(low_all, values, zero), jnp.where(low_all, one, zero)], axis=1
    )
    high_values = jnp.concatenate(
        [jnp.where(low_all, zero, values), jnp.where(low_all, zero, one)], axis=1
    )
    common, fresh, own = slice(0, 3 * rows), slice(3 * rows, 4 * rows), slice(4 * rows, 5 * rows)
    lanes = pl.ds(pl.multiple_of(pair * LANES, LANES), LANES)
    mine = q0_ref[part, lanes]
    others = jnp.concatenate([ref[part, lanes] for ref in (q1_ref, q2_ref, q3_ref)], 0)

    def halves(x):
        low_part = lax.broadcasted_iota(jnp.int32, x.shape, 1) < HEAD_DIM
        return jnp.concatenate([jnp.where(low_part, x, zero), jnp.where(low_part, zero, x)], 0)

    mine, others = halves(mine), halves(others)
    shared = scores_of(jnp.concatenate([mine, others], 0), keys[common])
    single = jnp.concatenate([scores_of(mine, keys[fresh]), scores_of(others, keys[own])], 0)
    top = single
    for index in range(3):
        top = jnp.maximum(top, shared[:, index * LANES : (index + 1) * LANES])
    top = jnp.max(top, -1, keepdims=True)
    shared = jnp.exp(shared - top).astype(BF16)
    single = jnp.exp(single - top).astype(BF16)

    def paired(x):
        return (
            jnp.concatenate([x[:rows], x[2 * rows : 5 * rows]], 0),
            jnp.concatenate([x[rows : 2 * rows], x[5 * rows :]], 0),
        )

    summed = jnp.dot(
        jnp.concatenate(paired(shared), 1),
        jnp.concatenate([low_values[common], high_values[common]], 0),
        preferred_element_type=F32,
    )
    single = jnp.concatenate(paired(single), 1)
    summed = summed + jnp.concatenate(
        [
            jnp.dot(
                single[:rows],
                jnp.concatenate([low_values[fresh], high_values[fresh]], 0),
                preferred_element_type=F32,
            ),
            jnp.dot(
                single[rows:],
                jnp.concatenate([low_values[own], high_values[own]], 0),
                preferred_element_type=F32,
            ),
        ],
        0,
    )
    total = summed[:, LANES:]
    mixed = (summed[:, :LANES] / total).astype(BF16)
    for index, o_ref in enumerate(out_refs):
        o_ref[:, lanes] = mixed[index * rows : (index + 1) * rows]
    lane = lax.broadcasted_iota(jnp.int32, total.shape, 1)
    low_top, high_top = paired(top)
    rest = jnp.where(lane < HEAD_DIM, low_top, high_top) + jnp.log(total)
    slot = lane & (HEAD_DIM - 1)
    tile = tile_scr[...]
    for piece in range(3):
        rounded = rest.astype(BF16).astype(F32)
        tile = jnp.where(slot == pair + piece * PIECES, rounded, tile)
        rest = rest - rounded
    tile_scr[...] = tile
    project(x_scr[...], wk_ref, wv_ref, kv_scr, 1 - current)

    @pl.when(pair == pl.num_programs(0) - 1)
    def _():
        if fetch:
            fetch.wait()
        for index, o_ref in enumerate(out_refs):
            o_ref[:, channels:] = tile_scr[index * rows : (index + 1) * rows, :].astype(BF16)


def spread_matrix(channels):
    out = np.zeros((LANES, channels), np.float32)
    for channel in range(channels):
        head = channel // HEAD_DIM
        base = (head % 2) * HEAD_DIM + head // 2
        for piece in range(3):
            out[base + piece * PIECES, channel] = 1
    return out


def exact_dot(x, ones):
    total = None
    for _ in range(3):
        rounded = x.astype(BF16)
        part = jnp.dot(rounded, ones, preferred_element_type=F32)
        total = part if total is None else total + part
        x = x - rounded.astype(F32)
    return total


def merge_kernel(
    o0_ref, o1_ref, o2_ref, o3_ref, hidden_ref, w_ref, spread_ref, gather_ref, *rest_refs, sample
):
    channels = hidden_ref.shape[1]
    rows = hidden_ref.shape[0]
    refs = (o0_ref, o1_ref, o2_ref, o3_ref)
    tiles = jnp.concatenate([ref[:, channels:] for ref in refs], 0)
    logs = jnp.dot(tiles, spread_ref[...], preferred_element_type=F32)
    logs = [logs[index * rows : (index + 1) * rows] for index in range(4)]
    top = jnp.maximum(jnp.maximum(logs[0], logs[1]), jnp.maximum(logs[2], logs[3]))
    numer = denom = None
    for ref, one in zip(refs, logs):
        factor = jnp.exp(one - top)
        upper = factor * ref[:, :channels].astype(F32)
        numer, denom = (upper, factor) if numer is None else (numer + upper, denom + factor)
    attended = (numer / denom).astype(BF16)
    residual = (
        hidden_ref[...].astype(F32) + jnp.dot(attended, w_ref[...], preferred_element_type=F32)
    ).astype(BF16)
    res_ref, stat_ref = rest_refs[-2:]
    res_ref[...] = residual
    wide = residual.astype(F32)
    sums = jnp.concatenate(
        [jnp.sum(wide, 0, keepdims=True), jnp.sum(wide * wide, 0, keepdims=True)]
        + [jnp.zeros((6, channels), F32)],
        0,
    )
    sums = exact_dot(sums, gather_ref[...])
    if sample:
        sums = pltpu.roll(sums, 2 * sample, 0) + rest_refs[0][...]
    stat_ref[...] = sums


def shifted(x, by, cols):
    rolled = pltpu.roll(x, by % x.shape[0], 0)
    col = lax.broadcasted_iota(jnp.int32, x.shape, 0) & (cols - 1)
    edge = 0 if by == 1 else cols - 1
    return jnp.where(col == edge, 0.0, rolled).astype(BF16)


def taps(x, weights, cols):
    wide = x.astype(F32)
    unfolded = jnp.concatenate([shifted(wide, 1, cols), x, shifted(wide, -1, cols)], 1)
    weights = weights.reshape(-1, weights.shape[-1])
    return jnp.dot(unfolded, weights, preferred_element_type=F32)


def rim_kernel(above_ref, below_ref, w_ref, bias_ref, shift_ref, out_ref, *, cols):
    total = taps(above_ref[...], w_ref[0], cols) + taps(below_ref[...], w_ref[2], cols)
    total += as_row(bias_ref)
    for sample in range(total.shape[0] // cols):
        part = slice(sample * cols, (sample + 1) * cols)
        out_ref[part, :] = total[part] + shift_ref[sample : sample + 1, :]


def add_kernel(*refs):
    refs[-1][...] = (refs[0][...] + refs[1][...]) + (refs[2][...] + refs[3][...])


def final_kernel(
    res0_ref, res1_ref, s0_ref, s1_ref, s2_ref, s3_ref, gain_ref, bias_ref, scatter_ref, w_ref, rim_ref, out_ref,
    *, cols, cells
):
    activated = []
    wide = []
    sums = (s0_ref[...] + s1_ref[...]) + (s2_ref[...] + s3_ref[...])
    sums = exact_dot(sums, scatter_ref[...])
    gain, bias = as_row(gain_ref), as_row(bias_ref)
    for sample, res_ref in enumerate((res0_ref, res1_ref)):
        mean = sums[2 * sample : 2 * sample + 1] / cells
        var = sums[2 * sample + 1 : 2 * sample + 2] / cells - mean * mean
        residual = res_ref[...].astype(F32)
        wide.append(residual)
        normalized = (residual - mean) * lax.rsqrt(var + EPSILON)
        value = normalized * gain + bias
        activated.append((value / (1.0 + jnp.exp(-value))).astype(BF16))
    x = jnp.concatenate(activated, 0)
    out_ref[...] = (
        taps(x, w_ref[1], cols) + rim_ref[...] + jnp.concatenate(wide, 0)
    ).astype(BF16)


def ring(by, count):
    return [(i, (i + by) % count) for i in range(count)]


def call(kernel, out_shape, *args, flops=1000000, chip=(), slow=(), **kwargs):
    spaces = {**dict.fromkeys(chip, pltpu.VMEM), **dict.fromkeys(slow, pltpu.HBM)}
    args = [
        pltpu.with_memory_space_constraint(x, spaces[index]) if index in spaces else x
        for index, x in enumerate(args)
    ]
    return pl.pallas_call(
        kernel,
        out_shape=out_shape,
        compiler_params=pltpu.CompilerParams(vmem_limit_bytes=24 * 2 ** 20),
        cost_estimate=pl.CostEstimate(flops=flops, bytes_accessed=1000000, transcendentals=0),
        **kwargs,
    )(*args)


def shards(
    hidden, stale_attn_in, stale_conv_in, ln_gain, ln_bias, w_qkv, w_out,
    gn_gain, gn_bias, conv_weight, conv_bias, time_shift,
):
    samples, rows_dev, cols, channels = hidden.shape
    tokens = rows_dev * cols
    every = samples * tokens
    pair_count = channels // LANES
    y_count, z_count = lax.axis_size("y"), lax.axis_size("z")
    count = y_count * z_count
    hid = hidden.reshape(every, channels)
    block = pltpu.VMEM((tokens, channels), BF16)
    full = pl.BlockSpec((every, channels), lambda i: (0, 0))
    vector = pl.BlockSpec((channels,), lambda i: (0,))
    shifts = (1, 3, 2)

    both = pltpu.VMEM((every, channels), BF16)
    stale = call(
        stale_norm_kernel, [block] * samples,
        stale_attn_in.reshape(every, channels), ln_gain, ln_bias,
        grid=(1,),
        in_specs=[full, vector, vector],
        out_specs=[VMEM] * samples,
        slow=(0, 1, 2),
        flops=6 * 10 ** 9,
    )
    along = []
    for s, one in enumerate(stale):
        up, down = (lax.ppermute(one, "z", ring(by, z_count)) for by in (1, 3))
        far = lax.ppermute(up, "z", ring(1, z_count)) if s % 2 == 0 else lax.ppermute(
            down, "z", ring(3, z_count)
        )
        along.append((up, far, down))
    queries, fresh = call(
        query_kernel, [both] * 2, hid, ln_gain, ln_bias, w_qkv,
        grid=(1,),
        in_specs=[VMEM, VMEM, VMEM, pl.BlockSpec((channels, channels), lambda i: (0, 0))],
        out_specs=[VMEM] * 2,
        flops=6 * 10 ** 9,
    )
    all_queries = [queries] + [lax.ppermute(queries, "y", ring(by, y_count)) for by in shifts]
    conv_rows = stale_conv_in.reshape(every, channels)
    above = lax.ppermute(conv_rows, ("y", "z"), [(i, i + 1) for i in range(count - 1)])
    below = lax.ppermute(conv_rows, ("y", "z"), [(i + 1, i) for i in range(count - 1)])

    wide = channels + LANES
    spread = jnp.asarray(spread_matrix(channels), BF16)
    group = np.arange(channels) // (channels // GROUPS)
    gather = group[:, None] == np.arange(LANES)[None, :]
    ext = pltpu.VMEM((tokens, wide), BF16)
    back = []
    for s in range(samples):
        extra = [pltpu.VMEM(conv_weight.shape, BF16)] * (s == samples - 1)
        outs = call(
            functools.partial(attend_kernel, sample=s), [ext] * 4 + extra,
            *all_queries, *along[s], fresh, stale[s],
            w_qkv, w_qkv, w_qkv, w_qkv, conv_weight,
            grid=(pair_count,),
            in_specs=[VMEM] * 9
            + [
                pl.BlockSpec((channels, LANES), lambda p: (0, pair_count)),
                pl.BlockSpec((channels, LANES), lambda p: (0, 2 * pair_count)),
                pl.BlockSpec((channels, LANES), lambda p: (0, jnp.minimum(pair_count + p + 1, 2 * pair_count - 1))),
                pl.BlockSpec((channels, LANES), lambda p: (0, jnp.minimum(2 * pair_count + p + 1, 3 * pair_count - 1))),
                pl.BlockSpec(memory_space=pl.ANY),
            ],
            out_specs=[VMEM] * (4 + len(extra)),
            scratch_shapes=[
                pltpu.VMEM((5 * tokens, channels), BF16),
                pltpu.VMEM((2, 5 * tokens, 2 * LANES), BF16),
                pltpu.VMEM((4 * tokens, LANES), F32),
                pltpu.SemaphoreType.DMA,
            ],
            flops=6 * 10 ** 9,
            chip=range(9),
            slow=(13,),
        )
        back.append(
            [outs[0]]
            + [lax.ppermute(one, "y", ring(-by, y_count)) for one, by in zip(outs[1:4], shifts)]
        )
    conv_on_chip = outs[4]
    rim = call(
        functools.partial(rim_kernel, cols=cols),
        pltpu.VMEM((every, channels), F32),
        above, below, conv_on_chip, conv_bias, time_shift,
        in_specs=[VMEM] * 5,
        out_specs=VMEM,
        flops=12 * every * channels * channels,
        chip=(0, 1, 2),
    )
    residuals, stats = [], []
    for s in range(samples):
        small = pltpu.VMEM((8, LANES), F32)
        res, stat = call(
            functools.partial(merge_kernel, sample=s), [block, small],
            *back[s], hid, w_out, spread, jnp.asarray(gather, BF16), *stats,
            grid=(1,),
            in_specs=[VMEM] * 4
            + [pl.BlockSpec((tokens, channels), lambda i, s=s: (s, 0))]
            + [VMEM] * (3 + len(stats)),
            out_specs=[VMEM, VMEM],
            flops=6 * 10 ** 9,
            chip=(0, 1, 2, 3, 5) + (8,) * s,
        )
        residuals.append(res)
        stats = [stat]
    stat = stats[0]
    along_y = [stat] + [lax.ppermute(stat, "y", ring(by, y_count)) for by in shifts]
    stat = call(add_kernel, small, *along_y, in_specs=[VMEM] * 4, out_specs=VMEM, chip=range(4))
    along_z = [stat] + [lax.ppermute(stat, "z", ring(by, z_count)) for by in shifts]
    out = call(
        functools.partial(
            final_kernel, cols=cols, cells=float(count * tokens * (channels // GROUPS))
        ),
        jax.ShapeDtypeStruct((every, channels), BF16),
        *residuals, *along_z, gn_gain, gn_bias, jnp.asarray(gather.T, BF16), conv_on_chip, rim,
        in_specs=[VMEM] * 11,
        out_specs=VMEM,
        chip=(0, 1, 2, 3, 4, 5, 9, 10),
        flops=6 * every * channels * channels,
    )
    return out.reshape(hidden.shape)


def solution(mesh):
    split = Mesh(mesh.devices.reshape(mesh.shape["img"], 4, 4), ("img", "y", "z"))
    rows = P("img", ("y", "z"), None, None)

    return jax.shard_map(
        shards,
        mesh=split,
        in_specs=(rows, rows, rows, P(), P(), P(), P(), P(), P(), P(), P(), P("img", None)),
        out_specs=rows,
        check_vma=False,
    )
```

```python
import functools

import jax
import jax.numpy as jnp
import numpy as np
from jax import lax
from jax.experimental import pallas as pl
from jax.experimental.pallas import tpu as pltpu
from jax.sharding import Mesh
from jax.sharding import PartitionSpec as P

GROUPS = 32
HEAD_DIM = 64
EPSILON = 1e-05
LANES = 128
PIECES = 8


F32 = jnp.float32
BF16 = jnp.bfloat16
VMEM = pl.BlockSpec(memory_space=pltpu.VMEM)


def normalize(values, gain, bias):
    values = values.astype(F32)
    centre = jnp.mean(values, -1, keepdims=True)
    centred = values - centre
    spread = jnp.mean(centred * centred, -1, keepdims=True)
    return (centred * lax.rsqrt(spread + EPSILON) * gain + bias).astype(BF16)


def as_row(ref):
    return ref[...].reshape(1, -1)


def stale_norm_kernel(x_ref, gain_ref, bias_ref, *out_refs):
    normed = normalize(x_ref[...], as_row(gain_ref), as_row(bias_ref))
    rows = out_refs[0].shape[0]
    for index, out_ref in enumerate(out_refs):
        out_ref[...] = normed[index * rows : (index + 1) * rows]


def query_kernel(x_ref, gain_ref, bias_ref, w_ref, q_ref, normed_ref):
    normed = normalize(x_ref[...], as_row(gain_ref), as_row(bias_ref))
    normed_ref[...] = normed
    projected = jnp.dot(normed, w_ref[...], preferred_element_type=F32).astype(BF16)
    q_ref[...] = (projected.astype(F32) * HEAD_DIM ** (-0.5)).astype(BF16)


def scores_of(queries, keys):
    return lax.dot_general(
        queries, keys, (((1,), (1,)), ((), ())), preferred_element_type=F32
    )


def project(x, wk_ref, wv_ref):
    weights = jnp.concatenate([wk_ref[...], wv_ref[...]], axis=1)
    return jnp.dot(x, weights, preferred_element_type=F32).astype(BF16)


def early_kernel(*refs):
    fresh_ref, *stale_refs, wk_ref, wv_ref, out_ref, x_scr = refs
    rows = stale_refs[0].shape[0]

    @pl.when(pl.program_id(0) == 0)
    def _():
        for sample, ref in enumerate(stale_refs):
            base = 2 * sample * rows
            x_scr[base : base + rows, :] = fresh_ref[sample * rows : (sample + 1) * rows, :]
            x_scr[base + rows : base + 2 * rows, :] = ref[...]

    lanes = pl.ds(pl.multiple_of(pl.program_id(0) * 2 * LANES, LANES), 2 * LANES)
    out_ref[:, lanes] = project(x_scr[...], wk_ref, wv_ref)


def attend_kernel(
    q0_ref, q1_ref, q2_ref, q3_ref,
    z1_ref, z2_ref, z3_ref, early_ref,
    wk0_ref, wv0_ref, wk_ref, wv_ref, conv_ref,
    o0_ref, o1_ref, o2_ref, o3_ref,
    *refs, sample,
):
    x_scr, kv_scr, tile_scr = refs[-4:-1]
    pair = pl.program_id(0)
    fetch = pltpu.make_async_copy(conv_ref, refs[0], refs[-1]) if len(refs) > 4 else None
    rows, channels = z2_ref.shape
    part = slice(sample * rows, (sample + 1) * rows)
    out_refs = (o0_ref, o1_ref, o2_ref, o3_ref)

    @pl.when(pair == 0)
    def _():
        if fetch:
            fetch.start()
        for index, ref in enumerate((z1_ref, z2_ref, z3_ref)):
            x_scr[index * rows : (index + 1) * rows, :] = ref[...]
        tile_scr[...] = jnp.zeros_like(tile_scr)
        kv_scr[0] = project(x_scr[...], wk0_ref, wv0_ref)

    current = pair & 1
    both_lanes = pl.ds(pl.multiple_of(pair * 2 * LANES, LANES), 2 * LANES)
    early = early_ref[2 * sample * rows : 2 * (sample + 1) * rows, both_lanes]
    pairs = jnp.concatenate([kv_scr[current], early], 0)
    keys, values = pairs[:, :LANES], pairs[:, LANES:]
    low_all = lax.broadcasted_iota(jnp.int32, keys.shape, 1) < HEAD_DIM
    zero = jnp.zeros((), BF16)
    one = jnp.ones((), BF16)
    low_values = jnp.concatenate(
        [jnp.where(low_all, values, zero), jnp.where(low_all, one, zero)], axis=1
    )
    high_values = jnp.concatenate(
        [jnp.where(low_all, zero, values), jnp.where(low_all, zero, one)], axis=1
    )
    common, fresh, own = slice(0, 3 * rows), slice(3 * rows, 4 * rows), slice(4 * rows, 5 * rows)
    lanes = pl.ds(pl.multiple_of(pair * LANES, LANES), LANES)
    mine = q0_ref[part, lanes]
    others = jnp.concatenate([ref[part, lanes] for ref in (q1_ref, q2_ref, q3_ref)], 0)

    def halves(x):
        low_part = lax.broadcasted_iota(jnp.int32, x.shape, 1) < HEAD_DIM
        return jnp.concatenate([jnp.where(low_part, x, zero), jnp.where(low_part, zero, x)], 0)

    mine, others = halves(mine), halves(others)
    scores = jnp.concatenate(
        [
            scores_of(mine, keys[: 4 * rows]),
            scores_of(others, jnp.concatenate([keys[common], keys[own]], 0)),
        ],
        0,
    )
    top = jnp.max(scores, -1, keepdims=True)
    scores = jnp.exp(scores - top).astype(BF16)
    shared, single = scores[:, : 3 * rows], scores[:, 3 * rows :]

    def paired(x):
        return (
            jnp.concatenate([x[:rows], x[2 * rows : 5 * rows]], 0),
            jnp.concatenate([x[rows : 2 * rows], x[5 * rows :]], 0),
        )

    summed = jnp.dot(
        jnp.concatenate(paired(shared), 1),
        jnp.concatenate([low_values[common], high_values[common]], 0),
        preferred_element_type=F32,
    )
    single = jnp.concatenate(paired(single), 1)
    summed = summed + jnp.concatenate(
        [
            jnp.dot(
                single[:rows],
                jnp.concatenate([low_values[fresh], high_values[fresh]], 0),
                preferred_element_type=F32,
            ),
            jnp.dot(
                single[rows:],
                jnp.concatenate([low_values[own], high_values[own]], 0),
                preferred_element_type=F32,
            ),
        ],
        0,
    )
    total = summed[:, LANES:]
    mixed = (summed[:, :LANES] / total).astype(BF16)
    for index, o_ref in enumerate(out_refs):
        o_ref[:, lanes] = mixed[index * rows : (index + 1) * rows]
    lane = lax.broadcasted_iota(jnp.int32, total.shape, 1)
    low_top, high_top = paired(top)
    rest = jnp.where(lane < HEAD_DIM, low_top, high_top) + jnp.log(total)
    slot = lane & (HEAD_DIM - 1)
    tile = tile_scr[...]
    for piece in range(3):
        rounded = rest.astype(BF16).astype(F32)
        tile = jnp.where(slot == pair + piece * PIECES, rounded, tile)
        rest = rest - rounded
    tile_scr[...] = tile
    kv_scr[1 - current] = project(x_scr[...], wk_ref, wv_ref)

    @pl.when(pair == pl.num_programs(0) - 1)
    def _():
        if fetch:
            fetch.wait()
        for index, o_ref in enumerate(out_refs):
            o_ref[:, channels:] = tile_scr[index * rows : (index + 1) * rows, :].astype(BF16)


def spread_matrix(channels):
    out = np.zeros((LANES, channels), np.float32)
    for channel in range(channels):
        head = channel // HEAD_DIM
        base = (head % 2) * HEAD_DIM + head // 2
        for piece in range(3):
            out[base + piece * PIECES, channel] = 1
    return out


def exact_dot(x, ones):
    total = None
    for _ in range(3):
        rounded = x.astype(BF16)
        part = jnp.dot(rounded, ones, preferred_element_type=F32)
        total = part if total is None else total + part
        x = x - rounded.astype(F32)
    return total


def merge_kernel(
    o0_ref, o1_ref, o2_ref, o3_ref, hidden_ref, w_ref, spread_ref, gather_ref, *rest_refs, sample
):
    channels = hidden_ref.shape[1]
    rows = hidden_ref.shape[0]
    refs = (o0_ref, o1_ref, o2_ref, o3_ref)
    tiles = jnp.concatenate([ref[:, channels:] for ref in refs], 0)
    logs = jnp.dot(tiles, spread_ref[...], preferred_element_type=F32)
    logs = [logs[index * rows : (index + 1) * rows] for index in range(4)]
    top = jnp.maximum(jnp.maximum(logs[0], logs[1]), jnp.maximum(logs[2], logs[3]))
    numer = denom = None
    for ref, one in zip(refs, logs):
        factor = jnp.exp(one - top)
        upper = factor * ref[:, :channels].astype(F32)
        numer, denom = (upper, factor) if numer is None else (numer + upper, denom + factor)
    attended = (numer / denom).astype(BF16)
    residual = (
        hidden_ref[...].astype(F32) + jnp.dot(attended, w_ref[...], preferred_element_type=F32)
    ).astype(BF16)
    res_ref, stat_ref = rest_refs[-2:]
    res_ref[...] = residual
    wide = residual.astype(F32)
    sums = jnp.concatenate(
        [jnp.sum(wide, 0, keepdims=True), jnp.sum(wide * wide, 0, keepdims=True)]
        + [jnp.zeros((6, channels), F32)],
        0,
    )
    sums = exact_dot(sums, gather_ref[...])
    if sample:
        sums = pltpu.roll(sums, 2 * sample, 0) + rest_refs[0][...]
    stat_ref[...] = sums


def shifted(x, by, cols):
    rolled = pltpu.roll(x, by % x.shape[0], 0)
    col = lax.broadcasted_iota(jnp.int32, x.shape, 0) & (cols - 1)
    edge = 0 if by == 1 else cols - 1
    return jnp.where(col == edge, 0.0, rolled).astype(BF16)


def taps(x, weights, cols):
    wide = x.astype(F32)
    unfolded = jnp.concatenate([shifted(wide, 1, cols), x, shifted(wide, -1, cols)], 1)
    weights = weights.reshape(-1, weights.shape[-1])
    return jnp.dot(unfolded, weights, preferred_element_type=F32)


def rim_kernel(above_ref, below_ref, w_ref, bias_ref, shift_ref, out_ref, *, cols):
    total = taps(above_ref[...], w_ref[0], cols) + taps(below_ref[...], w_ref[2], cols)
    total += as_row(bias_ref)
    for sample in range(total.shape[0] // cols):
        part = slice(sample * cols, (sample + 1) * cols)
        out_ref[part, :] = total[part] + shift_ref[sample : sample + 1, :]


def add_kernel(*refs):
    refs[-1][...] = (refs[0][...] + refs[1][...]) + (refs[2][...] + refs[3][...])


def final_kernel(
    res0_ref, res1_ref, s0_ref, s1_ref, s2_ref, s3_ref, gain_ref, bias_ref, scatter_ref, w_ref, rim_ref, out_ref,
    *, cols, cells
):
    activated = []
    wide = []
    sums = (s0_ref[...] + s1_ref[...]) + (s2_ref[...] + s3_ref[...])
    sums = exact_dot(sums, scatter_ref[...])
    gain, bias = as_row(gain_ref), as_row(bias_ref)
    for sample, res_ref in enumerate((res0_ref, res1_ref)):
        mean = sums[2 * sample : 2 * sample + 1] / cells
        var = sums[2 * sample + 1 : 2 * sample + 2] / cells - mean * mean
        residual = res_ref[...].astype(F32)
        wide.append(residual)
        normalized = (residual - mean) * lax.rsqrt(var + EPSILON)
        value = normalized * gain + bias
        activated.append((value / (1.0 + jnp.exp(-value))).astype(BF16))
    x = jnp.concatenate(activated, 0)
    out_ref[...] = (
        taps(x, w_ref[1], cols) + rim_ref[...] + jnp.concatenate(wide, 0)
    ).astype(BF16)


def ring(by, count):
    return [(i, (i + by) % count) for i in range(count)]


def call(kernel, out_shape, *args, flops=1000000, chip=(), slow=(), **kwargs):
    spaces = {**dict.fromkeys(chip, pltpu.VMEM), **dict.fromkeys(slow, pltpu.HBM)}
    args = [
        pltpu.with_memory_space_constraint(x, spaces[index]) if index in spaces else x
        for index, x in enumerate(args)
    ]
    return pl.pallas_call(
        kernel,
        out_shape=out_shape,
        compiler_params=pltpu.CompilerParams(vmem_limit_bytes=24 * 2 ** 20),
        cost_estimate=pl.CostEstimate(flops=flops, bytes_accessed=1000000, transcendentals=0),
        **kwargs,
    )(*args)


def shards(
    hidden, stale_attn_in, stale_conv_in, ln_gain, ln_bias, w_qkv, w_out,
    gn_gain, gn_bias, conv_weight, conv_bias, time_shift,
):
    samples, rows_dev, cols, channels = hidden.shape
    tokens = rows_dev * cols
    every = samples * tokens
    pair_count = channels // LANES
    y_count, z_count = lax.axis_size("y"), lax.axis_size("z")
    count = y_count * z_count
    hid = hidden.reshape(every, channels)
    block = pltpu.VMEM((tokens, channels), BF16)
    full = pl.BlockSpec((every, channels), lambda i: (0, 0))
    vector = pl.BlockSpec((channels,), lambda i: (0,))
    shifts = (1, 3, 2)

    both = pltpu.VMEM((every, channels), BF16)
    stale = call(
        stale_norm_kernel, [block] * samples,
        stale_attn_in.reshape(every, channels), ln_gain, ln_bias,
        grid=(1,),
        in_specs=[full, vector, vector],
        out_specs=[VMEM] * samples,
        slow=(0, 1, 2),
        flops=6 * 10 ** 9,
    )
    along = []
    for s, one in enumerate(stale):
        up, down = (lax.ppermute(one, "z", ring(by, z_count)) for by in (1, 3))
        far = lax.ppermute(up, "z", ring(1, z_count)) if s % 2 == 0 else lax.ppermute(
            down, "z", ring(3, z_count)
        )
        along.append((up, far, down))
    queries, fresh = call(
        query_kernel, [both] * 2, hid, ln_gain, ln_bias, w_qkv,
        grid=(1,),
        in_specs=[VMEM, VMEM, VMEM, pl.BlockSpec((channels, channels), lambda i: (0, 0))],
        out_specs=[VMEM] * 2,
        flops=6 * 10 ** 9,
    )
    all_queries = [queries] + [lax.ppermute(queries, "y", ring(by, y_count)) for by in shifts]
    early = call(
        early_kernel, pltpu.VMEM((2 * every, 2 * channels), BF16),
        fresh, *stale, w_qkv, w_qkv,
        grid=(pair_count,),
        in_specs=[VMEM] * (1 + samples)
        + [
            pl.BlockSpec((channels, LANES), lambda p: (0, pair_count + p)),
            pl.BlockSpec((channels, LANES), lambda p: (0, 2 * pair_count + p)),
        ],
        out_specs=VMEM,
        scratch_shapes=[pltpu.VMEM((2 * every, channels), BF16)],
        chip=range(1 + samples),
        flops=6 * 10 ** 9,
    )
    conv_rows = stale_conv_in.reshape(every, channels)
    above = lax.ppermute(conv_rows, ("y", "z"), [(i, i + 1) for i in range(count - 1)])
    below = lax.ppermute(conv_rows, ("y", "z"), [(i + 1, i) for i in range(count - 1)])

    wide = channels + LANES
    spread = jnp.asarray(spread_matrix(channels), BF16)
    group = np.arange(channels) // (channels // GROUPS)
    gather = group[:, None] == np.arange(LANES)[None, :]
    ext = pltpu.VMEM((tokens, wide), BF16)
    back = []
    for s in range(samples):
        extra = [pltpu.VMEM(conv_weight.shape, BF16)] * (s == samples - 1)
        outs = call(
            functools.partial(attend_kernel, sample=s), [ext] * 4 + extra,
            *all_queries, *along[s], early,
            w_qkv, w_qkv, w_qkv, w_qkv, conv_weight,
            grid=(pair_count,),
            in_specs=[VMEM] * 8
            + [
                pl.BlockSpec((channels, LANES), lambda p: (0, pair_count)),
                pl.BlockSpec((channels, LANES), lambda p: (0, 2 * pair_count)),
                pl.BlockSpec((channels, LANES), lambda p: (0, jnp.minimum(pair_count + p + 1, 2 * pair_count - 1))),
                pl.BlockSpec((channels, LANES), lambda p: (0, jnp.minimum(2 * pair_count + p + 1, 3 * pair_count - 1))),
                pl.BlockSpec(memory_space=pl.ANY),
            ],
            out_specs=[VMEM] * (4 + len(extra)),
            scratch_shapes=[
                pltpu.VMEM((3 * tokens, channels), BF16),
                pltpu.VMEM((2, 3 * tokens, 2 * LANES), BF16),
                pltpu.VMEM((4 * tokens, LANES), F32),
                pltpu.SemaphoreType.DMA,
            ],
            flops=6 * 10 ** 9,
            chip=range(8),
            slow=(12,),
        )
        back.append(
            [outs[0]]
            + [lax.ppermute(one, "y", ring(-by, y_count)) for one, by in zip(outs[1:4], shifts)]
        )
    conv_on_chip = outs[4]
    rim = call(
        functools.partial(rim_kernel, cols=cols),
        pltpu.VMEM((every, channels), F32),
        above, below, conv_on_chip, conv_bias, time_shift,
        in_specs=[VMEM] * 5,
        out_specs=VMEM,
        flops=12 * every * channels * channels,
        chip=(0, 1, 2),
    )
    residuals, stats = [], []
    for s in range(samples):
        small = pltpu.VMEM((8, LANES), F32)
        res, stat = call(
            functools.partial(merge_kernel, sample=s), [block, small],
            *back[s], hid, w_out, spread, jnp.asarray(gather, BF16), *stats,
            grid=(1,),
            in_specs=[VMEM] * 4
            + [pl.BlockSpec((tokens, channels), lambda i, s=s: (s, 0))]
            + [VMEM] * (3 + len(stats)),
            out_specs=[VMEM, VMEM],
            flops=6 * 10 ** 9,
            chip=(0, 1, 2, 3, 5) + (8,) * s,
        )
        residuals.append(res)
        stats = [stat]
    stat = stats[0]
    along_y = [stat] + [lax.ppermute(stat, "y", ring(by, y_count)) for by in shifts]
    stat = call(add_kernel, small, *along_y, in_specs=[VMEM] * 4, out_specs=VMEM, chip=range(4))
    along_z = [stat] + [lax.ppermute(stat, "z", ring(by, z_count)) for by in shifts]
    out = call(
        functools.partial(
            final_kernel, cols=cols, cells=float(count * tokens * (channels // GROUPS))
        ),
        jax.ShapeDtypeStruct((every, channels), BF16),
        *residuals, *along_z, gn_gain, gn_bias, jnp.asarray(gather.T, BF16), conv_on_chip, rim,
        in_specs=[VMEM] * 11,
        out_specs=VMEM,
        chip=(0, 1, 2, 3, 4, 5, 9, 10),
        flops=6 * every * channels * channels,
    )
    return out.reshape(hidden.shape)


def solution(mesh):
    split = Mesh(mesh.devices.reshape(mesh.shape["img"], 4, 4), ("img", "y", "z"))
    rows = P("img", ("y", "z"), None, None)

    return jax.shard_map(
        shards,
        mesh=split,
        in_specs=(rows, rows, rows, P(), P(), P(), P(), P(), P(), P(), P(), P("img", None)),
        out_specs=rows,
        check_vma=False,
    )
```

```python
import functools

import jax
import jax.numpy as jnp
import numpy as np
from jax import lax
from jax.experimental import pallas as pl
from jax.experimental.pallas import tpu as pltpu
from jax.sharding import Mesh
from jax.sharding import PartitionSpec as P

GROUPS = 32
HEAD_DIM = 64
EPSILON = 1e-05
LANES = 128
PIECES = 8


F32 = jnp.float32
BF16 = jnp.bfloat16
VMEM = pl.BlockSpec(memory_space=pltpu.VMEM)


def normalize(values, gain, bias):
    values = values.astype(F32)
    centre = jnp.mean(values, -1, keepdims=True)
    centred = values - centre
    spread = jnp.mean(centred * centred, -1, keepdims=True)
    return (centred * lax.rsqrt(spread + EPSILON) * gain + bias).astype(BF16)


def as_row(ref):
    return ref[...].reshape(1, -1)


def stale_norm_kernel(x_ref, gain_ref, bias_ref, *out_refs):
    normed = normalize(x_ref[...], as_row(gain_ref), as_row(bias_ref))
    rows = out_refs[0].shape[0]
    for index, out_ref in enumerate(out_refs):
        out_ref[...] = normed[index * rows : (index + 1) * rows]


def query_kernel(x_ref, gain_ref, bias_ref, w_ref, q_ref, normed_ref):
    normed = normalize(x_ref[...], as_row(gain_ref), as_row(bias_ref))
    normed_ref[...] = normed
    projected = jnp.dot(normed, w_ref[...], preferred_element_type=F32).astype(BF16)
    q_ref[...] = (projected.astype(F32) * HEAD_DIM ** (-0.5)).astype(BF16)


def scores_of(queries, keys):
    return lax.dot_general(
        queries, keys, (((1,), (1,)), ((), ())), preferred_element_type=F32
    )


def project(x, wk_ref, wv_ref):
    weights = jnp.concatenate([wk_ref[...], wv_ref[...]], axis=1)
    return jnp.dot(x, weights, preferred_element_type=F32).astype(BF16)


def early_kernel(*refs):
    fresh_ref, *stale_refs, wk_ref, wv_ref, out_ref, x_scr = refs
    rows = stale_refs[0].shape[0]

    @pl.when(pl.program_id(0) == 0)
    def _():
        for sample, ref in enumerate(stale_refs):
            base = 2 * sample * rows
            x_scr[base : base + rows, :] = fresh_ref[sample * rows : (sample + 1) * rows, :]
            x_scr[base + rows : base + 2 * rows, :] = ref[...]

    lanes = pl.ds(pl.multiple_of(pl.program_id(0) * 2 * LANES, LANES), 2 * LANES)
    out_ref[:, lanes] = project(x_scr[...], wk_ref, wv_ref)


def attend_kernel(
    q0_ref, q1_ref, q2_ref, q3_ref,
    z1_ref, z2_ref, z3_ref, early_ref,
    wk0_ref, wv0_ref, wk_ref, wv_ref, conv_ref,
    o0_ref, o1_ref, o2_ref, o3_ref,
    *refs, sample,
):
    x_scr, kv_scr, tile_scr = refs[-4:-1]
    pair = pl.program_id(0)
    fetch = pltpu.make_async_copy(conv_ref, refs[0], refs[-1]) if len(refs) > 4 else None
    rows, channels = z2_ref.shape
    part = slice(sample * rows, (sample + 1) * rows)
    out_refs = (o0_ref, o1_ref, o2_ref, o3_ref)

    @pl.when(pair == 0)
    def _():
        if fetch:
            fetch.start()
        for index, ref in enumerate((z1_ref, z2_ref, z3_ref)):
            x_scr[index * rows : (index + 1) * rows, :] = ref[...]
        tile_scr[...] = jnp.zeros_like(tile_scr)
        kv_scr[0] = project(x_scr[...], wk0_ref, wv0_ref)

    current = pair & 1
    both_lanes = pl.ds(pl.multiple_of(pair * 2 * LANES, LANES), 2 * LANES)
    early = early_ref[2 * sample * rows : 2 * (sample + 1) * rows, both_lanes]
    pairs = jnp.concatenate([kv_scr[current], early], 0)
    keys, values = pairs[:, :LANES], pairs[:, LANES:]
    low_all = lax.broadcasted_iota(jnp.int32, keys.shape, 1) < HEAD_DIM
    zero = jnp.zeros((), BF16)
    one = jnp.ones((), BF16)
    low_values = jnp.concatenate(
        [jnp.where(low_all, values, zero), jnp.where(low_all, one, zero)], axis=1
    )
    high_values = jnp.concatenate(
        [jnp.where(low_all, zero, values), jnp.where(low_all, zero, one)], axis=1
    )
    common, own = slice(0, 3 * rows), slice(4 * rows, 5 * rows)
    lanes = pl.ds(pl.multiple_of(pair * LANES, LANES), LANES)
    mine = q0_ref[part, lanes]
    others = [ref[part, lanes] for ref in (q1_ref, q2_ref, q3_ref)]

    own_keys, other_keys = keys[: 4 * rows], jnp.concatenate([keys[common], keys[own]], 0)
    low_part = lax.broadcasted_iota(jnp.int32, (rows, LANES), 1) < HEAD_DIM
    lows = [jnp.where(low_part, q, zero) for q in (mine, *others)]
    highs = [jnp.where(low_part, zero, q) for q in (mine, *others)]
    scores = [
        (scores_of(part[0], own_keys), scores_of(jnp.concatenate(part[1:], 0), other_keys))
        for part in (lows, highs)
    ]
    tops, sums = [], []
    for (first, rest), head_values in zip(scores, (low_values, high_values)):
        both = jnp.concatenate([first, rest], 0)
        top = jnp.max(both, -1, keepdims=True)
        both = jnp.exp(both - top).astype(BF16)
        tops.append(top)
        sums.append(
            jnp.concatenate(
                [
                    jnp.dot(both[:rows], head_values[: 4 * rows], preferred_element_type=F32),
                    jnp.dot(
                        both[rows:],
                        jnp.concatenate([head_values[common], head_values[own]], 0),
                        preferred_element_type=F32,
                    ),
                ],
                0,
            )
        )
    summed = sums[0] + sums[1]
    total = summed[:, LANES:]
    mixed = (summed[:, :LANES] / total).astype(BF16)
    for index, o_ref in enumerate(out_refs):
        o_ref[:, lanes] = mixed[index * rows : (index + 1) * rows]
    lane = lax.broadcasted_iota(jnp.int32, total.shape, 1)
    logs = jnp.where(lane < HEAD_DIM, tops[0], tops[1]) + jnp.log(total)
    tile_scr[...] = jnp.where((lane & (HEAD_DIM - 1)) == pair, logs, tile_scr[...])
    kv_scr[1 - current] = project(x_scr[...], wk_ref, wv_ref)

    @pl.when(pair == pl.num_programs(0) - 1)
    def _():
        if fetch:
            fetch.wait()
        rest = tile_scr[...]
        tile = jnp.zeros_like(rest)
        for piece in range(3):
            rounded = rest.astype(BF16).astype(F32)
            rest = rest - rounded
            tile = tile + (pltpu.roll(rounded, piece * PIECES, 1) if piece else rounded)
        for index, o_ref in enumerate(out_refs):
            o_ref[:, channels:] = tile[index * rows : (index + 1) * rows].astype(BF16)


def spread_matrix(channels):
    out = np.zeros((LANES, channels), np.float32)
    for channel in range(channels):
        head = channel // HEAD_DIM
        base = (head % 2) * HEAD_DIM + head // 2
        for piece in range(3):
            out[base + piece * PIECES, channel] = 1
    return out


def exact_dot(x, ones):
    total = None
    for _ in range(3):
        rounded = x.astype(BF16)
        part = jnp.dot(rounded, ones, preferred_element_type=F32)
        total = part if total is None else total + part
        x = x - rounded.astype(F32)
    return total


def merge_kernel(
    o0_ref, o1_ref, o2_ref, o3_ref, hidden_ref, w_ref, spread_ref, gather_ref, *rest_refs, sample
):
    channels = hidden_ref.shape[1]
    rows = hidden_ref.shape[0]
    refs = (o0_ref, o1_ref, o2_ref, o3_ref)
    tiles = jnp.concatenate([ref[:, channels:] for ref in refs], 0)
    logs = jnp.dot(tiles, spread_ref[...], preferred_element_type=F32)
    logs = [logs[index * rows : (index + 1) * rows] for index in range(4)]
    top = jnp.maximum(jnp.maximum(logs[0], logs[1]), jnp.maximum(logs[2], logs[3]))
    numer = denom = None
    for ref, one in zip(refs, logs):
        factor = jnp.exp(one - top)
        upper = factor * ref[:, :channels].astype(F32)
        numer, denom = (upper, factor) if numer is None else (numer + upper, denom + factor)
    attended = (numer / denom).astype(BF16)
    residual = (
        hidden_ref[...].astype(F32) + jnp.dot(attended, w_ref[...], preferred_element_type=F32)
    ).astype(BF16)
    res_ref, stat_ref = rest_refs[-2:]
    res_ref[...] = residual
    wide = residual.astype(F32)
    sums = jnp.concatenate(
        [jnp.sum(wide, 0, keepdims=True), jnp.sum(wide * wide, 0, keepdims=True)]
        + [jnp.zeros((6, channels), F32)],
        0,
    )
    sums = exact_dot(sums, gather_ref[...])
    if sample:
        sums = pltpu.roll(sums, 2 * sample, 0) + rest_refs[0][...]
    stat_ref[...] = sums


def shifted(x, by, cols):
    rolled = pltpu.roll(x, by % x.shape[0], 0)
    col = lax.broadcasted_iota(jnp.int32, x.shape, 0) & (cols - 1)
    edge = 0 if by == 1 else cols - 1
    return jnp.where(col == edge, 0.0, rolled).astype(BF16)


def taps(x, weights, cols):
    wide = x.astype(F32)
    unfolded = jnp.concatenate([shifted(wide, 1, cols), x, shifted(wide, -1, cols)], 1)
    weights = weights.reshape(-1, weights.shape[-1])
    return jnp.dot(unfolded, weights, preferred_element_type=F32)


def rim_kernel(above_ref, below_ref, w_ref, bias_ref, shift_ref, out_ref, *, cols):
    total = taps(above_ref[...], w_ref[0], cols) + taps(below_ref[...], w_ref[2], cols)
    total += as_row(bias_ref)
    for sample in range(total.shape[0] // cols):
        part = slice(sample * cols, (sample + 1) * cols)
        out_ref[part, :] = total[part] + shift_ref[sample : sample + 1, :]


def add_kernel(*refs):
    refs[-1][...] = (refs[0][...] + refs[1][...]) + (refs[2][...] + refs[3][...])


def final_kernel(
    res0_ref, res1_ref, s0_ref, s1_ref, s2_ref, s3_ref, gain_ref, bias_ref, scatter_ref, w_ref, rim_ref, out_ref,
    *, cols, cells
):
    activated = []
    wide = []
    sums = (s0_ref[...] + s1_ref[...]) + (s2_ref[...] + s3_ref[...])
    sums = exact_dot(sums, scatter_ref[...])
    gain, bias = as_row(gain_ref), as_row(bias_ref)
    for sample, res_ref in enumerate((res0_ref, res1_ref)):
        mean = sums[2 * sample : 2 * sample + 1] / cells
        var = sums[2 * sample + 1 : 2 * sample + 2] / cells - mean * mean
        residual = res_ref[...].astype(F32)
        wide.append(residual)
        normalized = (residual - mean) * lax.rsqrt(var + EPSILON)
        value = normalized * gain + bias
        activated.append((value / (1.0 + jnp.exp(-value))).astype(BF16))
    x = jnp.concatenate(activated, 0)
    out_ref[...] = (
        taps(x, w_ref[1], cols) + rim_ref[...] + jnp.concatenate(wide, 0)
    ).astype(BF16)


def ring(by, count):
    return [(i, (i + by) % count) for i in range(count)]


def call(kernel, out_shape, *args, flops=1000000, chip=(), slow=(), **kwargs):
    spaces = {**dict.fromkeys(chip, pltpu.VMEM), **dict.fromkeys(slow, pltpu.HBM)}
    args = [
        pltpu.with_memory_space_constraint(x, spaces[index]) if index in spaces else x
        for index, x in enumerate(args)
    ]
    return pl.pallas_call(
        kernel,
        out_shape=out_shape,
        compiler_params=pltpu.CompilerParams(vmem_limit_bytes=24 * 2 ** 20),
        cost_estimate=pl.CostEstimate(flops=flops, bytes_accessed=1000000, transcendentals=0),
        **kwargs,
    )(*args)


def shards(
    hidden, stale_attn_in, stale_conv_in, ln_gain, ln_bias, w_qkv, w_out,
    gn_gain, gn_bias, conv_weight, conv_bias, time_shift,
):
    samples, rows_dev, cols, channels = hidden.shape
    tokens = rows_dev * cols
    every = samples * tokens
    pair_count = channels // LANES
    y_count, z_count = lax.axis_size("y"), lax.axis_size("z")
    count = y_count * z_count
    hid = hidden.reshape(every, channels)
    block = pltpu.VMEM((tokens, channels), BF16)
    full = pl.BlockSpec((every, channels), lambda i: (0, 0))
    vector = pl.BlockSpec((channels,), lambda i: (0,))
    shifts = (1, 3, 2)

    both = pltpu.VMEM((every, channels), BF16)
    stale = call(
        stale_norm_kernel, [block] * samples,
        stale_attn_in.reshape(every, channels), ln_gain, ln_bias,
        grid=(1,),
        in_specs=[full, vector, vector],
        out_specs=[VMEM] * samples,
        slow=(0, 1, 2),
        flops=6 * 10 ** 9,
    )
    along = []
    for s, one in enumerate(stale):
        up, down = (lax.ppermute(one, "z", ring(by, z_count)) for by in (1, 3))
        far = lax.ppermute(up, "z", ring(1, z_count)) if s % 2 == 0 else lax.ppermute(
            down, "z", ring(3, z_count)
        )
        along.append((up, far, down))
    queries, fresh = call(
        query_kernel, [both] * 2, hid, ln_gain, ln_bias, w_qkv,
        grid=(1,),
        in_specs=[VMEM, VMEM, VMEM, pl.BlockSpec((channels, channels), lambda i: (0, 0))],
        out_specs=[VMEM] * 2,
        flops=6 * 10 ** 9,
    )
    all_queries = [queries] + [lax.ppermute(queries, "y", ring(by, y_count)) for by in shifts]
    early = call(
        early_kernel, pltpu.VMEM((2 * every, 2 * channels), BF16),
        fresh, *stale, w_qkv, w_qkv,
        grid=(pair_count,),
        in_specs=[VMEM] * (1 + samples)
        + [
            pl.BlockSpec((channels, LANES), lambda p: (0, pair_count + p)),
            pl.BlockSpec((channels, LANES), lambda p: (0, 2 * pair_count + p)),
        ],
        out_specs=VMEM,
        scratch_shapes=[pltpu.VMEM((2 * every, channels), BF16)],
        chip=range(1 + samples),
        flops=6 * 10 ** 9,
    )
    conv_rows = stale_conv_in.reshape(every, channels)
    above = lax.ppermute(conv_rows, ("y", "z"), [(i, i + 1) for i in range(count - 1)])
    below = lax.ppermute(conv_rows, ("y", "z"), [(i + 1, i) for i in range(count - 1)])

    wide = channels + LANES
    spread = jnp.asarray(spread_matrix(channels), BF16)
    group = np.arange(channels) // (channels // GROUPS)
    gather = group[:, None] == np.arange(LANES)[None, :]
    ext = pltpu.VMEM((tokens, wide), BF16)
    back = []
    for s in range(samples):
        extra = [pltpu.VMEM(conv_weight.shape, BF16)] * (s == samples - 1)
        outs = call(
            functools.partial(attend_kernel, sample=s), [ext] * 4 + extra,
            *all_queries, *along[s], early,
            w_qkv, w_qkv, w_qkv, w_qkv, conv_weight,
            grid=(pair_count,),
            in_specs=[VMEM] * 8
            + [
                pl.BlockSpec((channels, LANES), lambda p: (0, pair_count)),
                pl.BlockSpec((channels, LANES), lambda p: (0, 2 * pair_count)),
                pl.BlockSpec((channels, LANES), lambda p: (0, jnp.minimum(pair_count + p + 1, 2 * pair_count - 1))),
                pl.BlockSpec((channels, LANES), lambda p: (0, jnp.minimum(2 * pair_count + p + 1, 3 * pair_count - 1))),
                pl.BlockSpec(memory_space=pl.ANY),
            ],
            out_specs=[VMEM] * (4 + len(extra)),
            scratch_shapes=[
                pltpu.VMEM((3 * tokens, channels), BF16),
                pltpu.VMEM((2, 3 * tokens, 2 * LANES), BF16),
                pltpu.VMEM((4 * tokens, LANES), F32),
                pltpu.SemaphoreType.DMA,
            ],
            flops=6 * 10 ** 9,
            chip=range(8),
            slow=(12,),
        )
        back.append(
            [outs[0]]
            + [lax.ppermute(one, "y", ring(-by, y_count)) for one, by in zip(outs[1:4], shifts)]
        )
    conv_on_chip = outs[4]
    rim = call(
        functools.partial(rim_kernel, cols=cols),
        pltpu.VMEM((every, channels), F32),
        above, below, conv_on_chip, conv_bias, time_shift,
        in_specs=[VMEM] * 5,
        out_specs=VMEM,
        flops=12 * every * channels * channels,
        chip=(0, 1, 2),
    )
    residuals, stats = [], []
    for s in range(samples):
        small = pltpu.VMEM((8, LANES), F32)
        res, stat = call(
            functools.partial(merge_kernel, sample=s), [block, small],
            *back[s], hid, w_out, spread, jnp.asarray(gather, BF16), *stats,
            grid=(1,),
            in_specs=[VMEM] * 4
            + [pl.BlockSpec((tokens, channels), lambda i, s=s: (s, 0))]
            + [VMEM] * (3 + len(stats)),
            out_specs=[VMEM, VMEM],
            flops=6 * 10 ** 9,
            chip=(0, 1, 2, 3, 5) + (8,) * s,
        )
        residuals.append(res)
        stats = [stat]
    stat = stats[0]
    along_y = [stat] + [lax.ppermute(stat, "y", ring(by, y_count)) for by in shifts]
    stat = call(add_kernel, small, *along_y, in_specs=[VMEM] * 4, out_specs=VMEM, chip=range(4))
    along_z = [stat] + [lax.ppermute(stat, "z", ring(by, z_count)) for by in shifts]
    out = call(
        functools.partial(
            final_kernel, cols=cols, cells=float(count * tokens * (channels // GROUPS))
        ),
        jax.ShapeDtypeStruct((every, channels), BF16),
        *residuals, *along_z, gn_gain, gn_bias, jnp.asarray(gather.T, BF16), conv_on_chip, rim,
        in_specs=[VMEM] * 11,
        out_specs=VMEM,
        chip=(0, 1, 2, 3, 4, 5, 9, 10),
        flops=6 * every * channels * channels,
    )
    return out.reshape(hidden.shape)


def solution(mesh):
    split = Mesh(mesh.devices.reshape(mesh.shape["img"], 4, 4), ("img", "y", "z"))
    rows = P("img", ("y", "z"), None, None)

    return jax.shard_map(
        shards,
        mesh=split,
        in_specs=(rows, rows, rows, P(), P(), P(), P(), P(), P(), P(), P(), P("img", None)),
        out_specs=rows,
        check_vma=False,
    )
```

```python
import functools

import jax
import jax.numpy as jnp
import numpy as np
from jax import lax
from jax.experimental import pallas as pl
from jax.experimental.pallas import tpu as pltpu
from jax.sharding import Mesh
from jax.sharding import PartitionSpec as P

GROUPS = 32
HEAD_DIM = 64
EPSILON = 1e-05
LANES = 128
PIECES = 8


F32 = jnp.float32
BF16 = jnp.bfloat16
VMEM = pl.BlockSpec(memory_space=pltpu.VMEM)


def normalize(values, gain, bias):
    values = values.astype(F32)
    centre = jnp.mean(values, -1, keepdims=True)
    centred = values - centre
    spread = jnp.mean(centred * centred, -1, keepdims=True)
    return (centred * lax.rsqrt(spread + EPSILON) * gain + bias).astype(BF16)


def as_row(ref):
    return ref[...].reshape(1, -1)


def stale_norm_kernel(x_ref, gain_ref, bias_ref, *out_refs):
    normed = normalize(x_ref[...], as_row(gain_ref), as_row(bias_ref))
    rows = out_refs[0].shape[0]
    for index, out_ref in enumerate(out_refs):
        out_ref[...] = normed[index * rows : (index + 1) * rows]


def query_kernel(x_ref, gain_ref, bias_ref, w_ref, q_ref, normed_ref):
    normed = normalize(x_ref[...], as_row(gain_ref), as_row(bias_ref))
    normed_ref[...] = normed
    projected = jnp.dot(normed, w_ref[...], preferred_element_type=F32).astype(BF16)
    q_ref[...] = (projected.astype(F32) * HEAD_DIM ** (-0.5)).astype(BF16)


def scores_of(queries, keys):
    return lax.dot_general(
        queries, keys, (((1,), (1,)), ((), ())), preferred_element_type=F32
    )


def project(x, wk_ref, wv_ref):
    weights = jnp.concatenate([wk_ref[...], wv_ref[...]], axis=1)
    return jnp.dot(x, weights, preferred_element_type=F32).astype(BF16)


def early_kernel(*refs):
    fresh_ref, *stale_refs, wk_ref, wv_ref, out_ref, x_scr = refs
    rows = stale_refs[0].shape[0]

    @pl.when(pl.program_id(0) == 0)
    def _():
        for sample, ref in enumerate(stale_refs):
            base = 2 * sample * rows
            x_scr[base : base + rows, :] = fresh_ref[sample * rows : (sample + 1) * rows, :]
            x_scr[base + rows : base + 2 * rows, :] = ref[...]

    lanes = pl.ds(pl.multiple_of(pl.program_id(0) * 2 * LANES, LANES), 2 * LANES)
    out_ref[:, lanes] = project(x_scr[...], wk_ref, wv_ref)


def attend_kernel(
    q0_ref, q1_ref, q2_ref, q3_ref,
    z1_ref, z2_ref, z3_ref, early_ref,
    wk0_ref, wv0_ref, wk_ref, wv_ref, conv_ref,
    o0_ref, o1_ref, o2_ref, o3_ref,
    *refs, sample,
):
    x_scr, kv_scr, tile_scr = refs[-4:-1]
    pair = pl.program_id(0)
    fetch = pltpu.make_async_copy(conv_ref, refs[0], refs[-1]) if len(refs) > 4 else None
    rows, channels = z2_ref.shape
    part = slice(sample * rows, (sample + 1) * rows)
    out_refs = (o0_ref, o1_ref, o2_ref, o3_ref)

    @pl.when(pair == 0)
    def _():
        if fetch:
            fetch.start()
        for index, ref in enumerate((z1_ref, z2_ref, z3_ref)):
            x_scr[index * rows : (index + 1) * rows, :] = ref[...]
        tile_scr[...] = jnp.zeros_like(tile_scr)
        kv_scr[0] = project(x_scr[...], wk0_ref, wv0_ref)

    current = pair & 1
    both_lanes = pl.ds(pl.multiple_of(pair * 2 * LANES, LANES), 2 * LANES)
    early = early_ref[2 * sample * rows : 2 * (sample + 1) * rows, both_lanes]
    pairs = jnp.concatenate([kv_scr[current], early], 0)
    keys, values = pairs[:, :LANES], pairs[:, LANES:]
    low_all = lax.broadcasted_iota(jnp.int32, keys.shape, 1) < HEAD_DIM
    zero = jnp.zeros((), BF16)
    one = jnp.ones((), BF16)
    low_values = jnp.concatenate(
        [jnp.where(low_all, values, zero), jnp.where(low_all, one, zero)], axis=1
    )
    high_values = jnp.concatenate(
        [jnp.where(low_all, zero, values), jnp.where(low_all, zero, one)], axis=1
    )
    common, own = slice(0, 3 * rows), slice(4 * rows, 5 * rows)
    lanes = pl.ds(pl.multiple_of(pair * LANES, LANES), LANES)
    mine = q0_ref[part, lanes]
    others = [ref[part, lanes] for ref in (q1_ref, q2_ref, q3_ref)]

    own_keys, other_keys = keys[: 4 * rows], jnp.concatenate([keys[common], keys[own]], 0)
    low_part = lax.broadcasted_iota(jnp.int32, (rows, LANES), 1) < HEAD_DIM
    lows = [jnp.where(low_part, q, zero) for q in (mine, *others)]
    highs = [jnp.where(low_part, zero, q) for q in (mine, *others)]
    scores = [
        (scores_of(part[0], own_keys), scores_of(jnp.concatenate(part[1:], 0), other_keys))
        for part in (lows, highs)
    ]
    tops, sums = [], []
    for (first, rest), head_values in zip(scores, (low_values, high_values)):
        both = jnp.concatenate([first, rest], 0)
        top = jnp.max(both, -1, keepdims=True)
        both = jnp.exp(both - top).astype(BF16)
        tops.append(top)
        sums.append(
            jnp.concatenate(
                [
                    jnp.dot(both[:rows], head_values[: 4 * rows], preferred_element_type=F32),
                    jnp.dot(
                        both[rows:],
                        jnp.concatenate([head_values[common], head_values[own]], 0),
                        preferred_element_type=F32,
                    ),
                ],
                0,
            )
        )
    summed = sums[0] + sums[1]
    total = summed[:, LANES:]
    mixed = (summed[:, :LANES] / total).astype(BF16)
    for index, o_ref in enumerate(out_refs):
        o_ref[:, lanes] = mixed[index * rows : (index + 1) * rows]
    lane = lax.broadcasted_iota(jnp.int32, total.shape, 1)
    logs = jnp.where(lane < HEAD_DIM, tops[0], tops[1]) + jnp.log(total)
    tile_scr[...] = jnp.where((lane & (HEAD_DIM - 1)) == pair, logs, tile_scr[...])
    kv_scr[1 - current] = project(x_scr[...], wk_ref, wv_ref)

    @pl.when(pair == pl.num_programs(0) - 1)
    def _():
        if fetch:
            fetch.wait()
        rest = tile_scr[...]
        tile = jnp.zeros_like(rest)
        for piece in range(3):
            rounded = rest.astype(BF16).astype(F32)
            rest = rest - rounded
            tile = tile + (pltpu.roll(rounded, piece * PIECES, 1) if piece else rounded)
        for index, o_ref in enumerate(out_refs):
            o_ref[:, channels:] = tile[index * rows : (index + 1) * rows].astype(BF16)


def spread_matrix(channels):
    out = np.zeros((LANES, channels), np.float32)
    for channel in range(channels):
        head = channel // HEAD_DIM
        base = (head % 2) * HEAD_DIM + head // 2
        for piece in range(3):
            out[base + piece * PIECES, channel] = 1
    return out


def exact_dot(x, ones):
    total = None
    for _ in range(3):
        rounded = x.astype(BF16)
        part = jnp.dot(rounded, ones, preferred_element_type=F32)
        total = part if total is None else total + part
        x = x - rounded.astype(F32)
    return total


def merge_kernel(*refs):
    *o_refs, hidden_ref, w_ref, spread_ref, gather_ref, res_ref, stat_ref = refs
    channels = hidden_ref.shape[1]
    rows = o_refs[0].shape[0]
    samples = len(o_refs) // 4
    attended = []
    for sample in range(samples):
        parts = o_refs[4 * sample : 4 * sample + 4]
        tiles = jnp.concatenate([ref[:, channels:] for ref in parts], 0)
        logs = jnp.dot(tiles, spread_ref[...], preferred_element_type=F32)
        logs = [logs[index * rows : (index + 1) * rows] for index in range(4)]
        top = jnp.maximum(jnp.maximum(logs[0], logs[1]), jnp.maximum(logs[2], logs[3]))
        numer = denom = None
        for ref, one in zip(parts, logs):
            factor = jnp.exp(one - top)
            upper = factor * ref[:, :channels].astype(F32)
            numer, denom = (upper, factor) if numer is None else (numer + upper, denom + factor)
        attended.append((numer / denom).astype(BF16))
    residual = (
        hidden_ref[...].astype(F32)
        + jnp.dot(jnp.concatenate(attended, 0), w_ref[...], preferred_element_type=F32)
    ).astype(BF16)
    res_ref[...] = residual
    wide = residual.astype(F32)
    sums = []
    for sample in range(samples):
        part = wide[sample * rows : (sample + 1) * rows]
        sums += [jnp.sum(part, 0, keepdims=True), jnp.sum(part * part, 0, keepdims=True)]
    sums = jnp.concatenate(sums + [jnp.zeros((8 - len(sums), channels), F32)], 0)
    stat_ref[...] = exact_dot(sums, gather_ref[...])


def shifted(x, by, cols):
    rolled = pltpu.roll(x, by % x.shape[0], 0)
    col = lax.broadcasted_iota(jnp.int32, x.shape, 0) & (cols - 1)
    edge = 0 if by == 1 else cols - 1
    return jnp.where(col == edge, 0.0, rolled).astype(BF16)


def taps(x, weights, cols):
    wide = x.astype(F32)
    unfolded = jnp.concatenate([shifted(wide, 1, cols), x, shifted(wide, -1, cols)], 1)
    weights = weights.reshape(-1, weights.shape[-1])
    return jnp.dot(unfolded, weights, preferred_element_type=F32)


def rim_kernel(above_ref, below_ref, w_ref, bias_ref, shift_ref, out_ref, *, cols):
    total = taps(above_ref[...], w_ref[0], cols) + taps(below_ref[...], w_ref[2], cols)
    total += as_row(bias_ref)
    for sample in range(total.shape[0] // cols):
        part = slice(sample * cols, (sample + 1) * cols)
        out_ref[part, :] = total[part] + shift_ref[sample : sample + 1, :]


def add_kernel(*refs):
    refs[-1][...] = (refs[0][...] + refs[1][...]) + (refs[2][...] + refs[3][...])


def final_kernel(
    res_ref, s0_ref, s1_ref, s2_ref, s3_ref, gain_ref, bias_ref, scatter_ref, w_ref, rim_ref, out_ref,
    *, cols, cells
):
    activated = []
    sums = (s0_ref[...] + s1_ref[...]) + (s2_ref[...] + s3_ref[...])
    sums = exact_dot(sums, scatter_ref[...])
    gain, bias = as_row(gain_ref), as_row(bias_ref)
    wide = res_ref[...].astype(F32)
    for sample in range(wide.shape[0] // cols):
        mean = sums[2 * sample : 2 * sample + 1] / cells
        var = sums[2 * sample + 1 : 2 * sample + 2] / cells - mean * mean
        residual = wide[sample * cols : (sample + 1) * cols]
        normalized = (residual - mean) * lax.rsqrt(var + EPSILON)
        value = normalized * gain + bias
        activated.append((value / (1.0 + jnp.exp(-value))).astype(BF16))
    x = jnp.concatenate(activated, 0)
    out_ref[...] = (
        taps(x, w_ref[1], cols) + rim_ref[...] + wide
    ).astype(BF16)


def ring(by, count):
    return [(i, (i + by) % count) for i in range(count)]


def call(kernel, out_shape, *args, flops=1000000, chip=(), slow=(), **kwargs):
    spaces = {**dict.fromkeys(chip, pltpu.VMEM), **dict.fromkeys(slow, pltpu.HBM)}
    args = [
        pltpu.with_memory_space_constraint(x, spaces[index]) if index in spaces else x
        for index, x in enumerate(args)
    ]
    return pl.pallas_call(
        kernel,
        out_shape=out_shape,
        compiler_params=pltpu.CompilerParams(vmem_limit_bytes=24 * 2 ** 20),
        cost_estimate=pl.CostEstimate(flops=flops, bytes_accessed=1000000, transcendentals=0),
        **kwargs,
    )(*args)


def shards(
    hidden, stale_attn_in, stale_conv_in, ln_gain, ln_bias, w_qkv, w_out,
    gn_gain, gn_bias, conv_weight, conv_bias, time_shift,
):
    samples, rows_dev, cols, channels = hidden.shape
    tokens = rows_dev * cols
    every = samples * tokens
    pair_count = channels // LANES
    y_count, z_count = lax.axis_size("y"), lax.axis_size("z")
    count = y_count * z_count
    hid = hidden.reshape(every, channels)
    block = pltpu.VMEM((tokens, channels), BF16)
    full = pl.BlockSpec((every, channels), lambda i: (0, 0))
    vector = pl.BlockSpec((channels,), lambda i: (0,))
    shifts = (1, 3, 2)

    both = pltpu.VMEM((every, channels), BF16)
    stale = call(
        stale_norm_kernel, [block] * samples,
        stale_attn_in.reshape(every, channels), ln_gain, ln_bias,
        grid=(1,),
        in_specs=[full, vector, vector],
        out_specs=[VMEM] * samples,
        slow=(0, 1, 2),
        flops=6 * 10 ** 9,
    )
    along = []
    for s, one in enumerate(stale):
        up, down = (lax.ppermute(one, "z", ring(by, z_count)) for by in (1, 3))
        far = lax.ppermute(up, "z", ring(1, z_count)) if s % 2 == 0 else lax.ppermute(
            down, "z", ring(3, z_count)
        )
        along.append((up, far, down))
    queries, fresh = call(
        query_kernel, [both] * 2, hid, ln_gain, ln_bias, w_qkv,
        grid=(1,),
        in_specs=[VMEM, VMEM, VMEM, pl.BlockSpec((channels, channels), lambda i: (0, 0))],
        out_specs=[VMEM] * 2,
        flops=6 * 10 ** 9,
    )
    all_queries = [queries] + [lax.ppermute(queries, "y", ring(by, y_count)) for by in shifts]
    early = call(
        early_kernel, pltpu.VMEM((2 * every, 2 * channels), BF16),
        fresh, *stale, w_qkv, w_qkv,
        grid=(pair_count,),
        in_specs=[VMEM] * (1 + samples)
        + [
            pl.BlockSpec((channels, LANES), lambda p: (0, pair_count + p)),
            pl.BlockSpec((channels, LANES), lambda p: (0, 2 * pair_count + p)),
        ],
        out_specs=VMEM,
        scratch_shapes=[pltpu.VMEM((2 * every, channels), BF16)],
        chip=range(1 + samples),
        flops=6 * 10 ** 9,
    )
    conv_rows = stale_conv_in.reshape(every, channels)
    above = lax.ppermute(conv_rows, ("y", "z"), [(i, i + 1) for i in range(count - 1)])
    below = lax.ppermute(conv_rows, ("y", "z"), [(i + 1, i) for i in range(count - 1)])

    wide = channels + LANES
    spread = jnp.asarray(spread_matrix(channels), BF16)
    group = np.arange(channels) // (channels // GROUPS)
    gather = group[:, None] == np.arange(LANES)[None, :]
    ext = pltpu.VMEM((tokens, wide), BF16)
    back = []
    for s in range(samples):
        extra = [pltpu.VMEM(conv_weight.shape, BF16)] * (s == samples - 1)
        outs = call(
            functools.partial(attend_kernel, sample=s), [ext] * 4 + extra,
            *all_queries, *along[s], early,
            w_qkv, w_qkv, w_qkv, w_qkv, conv_weight,
            grid=(pair_count,),
            in_specs=[VMEM] * 8
            + [
                pl.BlockSpec((channels, LANES), lambda p: (0, pair_count)),
                pl.BlockSpec((channels, LANES), lambda p: (0, 2 * pair_count)),
                pl.BlockSpec((channels, LANES), lambda p: (0, jnp.minimum(pair_count + p + 1, 2 * pair_count - 1))),
                pl.BlockSpec((channels, LANES), lambda p: (0, jnp.minimum(2 * pair_count + p + 1, 3 * pair_count - 1))),
                pl.BlockSpec(memory_space=pl.ANY),
            ],
            out_specs=[VMEM] * (4 + len(extra)),
            scratch_shapes=[
                pltpu.VMEM((3 * tokens, channels), BF16),
                pltpu.VMEM((2, 3 * tokens, 2 * LANES), BF16),
                pltpu.VMEM((4 * tokens, LANES), F32),
                pltpu.SemaphoreType.DMA,
            ],
            flops=6 * 10 ** 9,
            chip=range(8),
            slow=(12,),
        )
        back.append(
            [outs[0]]
            + [lax.ppermute(one, "y", ring(-by, y_count)) for one, by in zip(outs[1:4], shifts)]
        )
    conv_on_chip = outs[4]
    rim = call(
        functools.partial(rim_kernel, cols=cols),
        pltpu.VMEM((every, channels), F32),
        above, below, conv_on_chip, conv_bias, time_shift,
        in_specs=[VMEM] * 5,
        out_specs=VMEM,
        flops=12 * every * channels * channels,
        chip=(0, 1, 2),
    )
    small = pltpu.VMEM((8, LANES), F32)
    residual, stat = call(
        merge_kernel, [both, small],
        *sum(back, []), hid, w_out, spread, jnp.asarray(gather, BF16),
        grid=(1,),
        in_specs=[VMEM] * (4 * samples + 4),
        out_specs=[VMEM, VMEM],
        flops=6 * 10 ** 9,
        chip=tuple(range(4 * samples)) + (4 * samples + 1,),
    )
    along_y = [stat] + [lax.ppermute(stat, "y", ring(by, y_count)) for by in shifts]
    stat = call(add_kernel, small, *along_y, in_specs=[VMEM] * 4, out_specs=VMEM, chip=range(4))
    along_z = [stat] + [lax.ppermute(stat, "z", ring(by, z_count)) for by in shifts]
    out = call(
        functools.partial(
            final_kernel, cols=cols, cells=float(count * tokens * (channels // GROUPS))
        ),
        jax.ShapeDtypeStruct((every, channels), BF16),
        residual, *along_z, gn_gain, gn_bias, jnp.asarray(gather.T, BF16), conv_on_chip, rim,
        in_specs=[VMEM] * 10,
        out_specs=VMEM,
        chip=(0, 1, 2, 3, 4, 8, 9),
        flops=6 * every * channels * channels,
    )
    return out.reshape(hidden.shape)


def solution(mesh):
    split = Mesh(mesh.devices.reshape(mesh.shape["img"], 4, 4), ("img", "y", "z"))
    rows = P("img", ("y", "z"), None, None)

    return jax.shard_map(
        shards,
        mesh=split,
        in_specs=(rows, rows, rows, P(), P(), P(), P(), P(), P(), P(), P(), P("img", None)),
        out_specs=rows,
        check_vma=False,
    )
```

```python
import functools

import jax
import jax.numpy as jnp
import numpy as np
from jax import lax
from jax.experimental import pallas as pl
from jax.experimental.pallas import tpu as pltpu
from jax.sharding import Mesh
from jax.sharding import PartitionSpec as P

GROUPS = 32
HEAD_DIM = 64
EPSILON = 1e-05
LANES = 128
PIECES = 8


F32 = jnp.float32
BF16 = jnp.bfloat16
VMEM = pl.BlockSpec(memory_space=pltpu.VMEM)


def normalize(values, gain, bias):
    values = values.astype(F32)
    centre = jnp.mean(values, -1, keepdims=True)
    centred = values - centre
    spread = jnp.mean(centred * centred, -1, keepdims=True)
    return (centred * lax.rsqrt(spread + EPSILON) * gain + bias).astype(BF16)


def as_row(ref):
    return ref[...].reshape(1, -1)


def stale_norm_kernel(x_ref, gain_ref, bias_ref, *out_refs):
    normed = normalize(x_ref[...], as_row(gain_ref), as_row(bias_ref))
    rows = out_refs[0].shape[0]
    for index, out_ref in enumerate(out_refs):
        out_ref[...] = normed[index * rows : (index + 1) * rows]


def query_kernel(x_ref, gain_ref, bias_ref, w_ref, q_ref, normed_ref):
    normed = normalize(x_ref[...], as_row(gain_ref), as_row(bias_ref))
    normed_ref[...] = normed
    projected = jnp.dot(normed, w_ref[...], preferred_element_type=F32).astype(BF16)
    q_ref[...] = (projected.astype(F32) * HEAD_DIM ** (-0.5)).astype(BF16)


def scores_of(queries, keys):
    return lax.dot_general(
        queries, keys, (((1,), (1,)), ((), ())), preferred_element_type=F32
    )


def project(x, wk_ref, wv_ref):
    weights = jnp.concatenate([wk_ref[...], wv_ref[...]], axis=1)
    return jnp.dot(x, weights, preferred_element_type=F32).astype(BF16)


def early_kernel(*refs):
    fresh_ref, *stale_refs, wk_ref, wv_ref, out_ref, x_scr = refs
    rows = stale_refs[0].shape[0]

    @pl.when(pl.program_id(0) == 0)
    def _():
        for sample, ref in enumerate(stale_refs):
            base = 2 * sample * rows
            x_scr[base : base + rows, :] = fresh_ref[sample * rows : (sample + 1) * rows, :]
            x_scr[base + rows : base + 2 * rows, :] = ref[...]

    lanes = pl.ds(pl.multiple_of(pl.program_id(0) * 2 * LANES, LANES), 2 * LANES)
    out_ref[:, lanes] = project(x_scr[...], wk_ref, wv_ref)


def attend_kernel(
    q0_ref, q1_ref, q2_ref, q3_ref,
    z1_ref, z2_ref, z3_ref, early_ref,
    wk0_ref, wv0_ref, wk_ref, wv_ref, conv_ref,
    o0_ref, o1_ref, o2_ref, o3_ref,
    *refs, sample,
):
    x_scr, kv_scr, tile_scr = refs[-4:-1]
    pair = pl.program_id(0)
    fetch = pltpu.make_async_copy(conv_ref, refs[0], refs[-1]) if len(refs) > 4 else None
    rows, channels = z2_ref.shape
    part = slice(sample * rows, (sample + 1) * rows)
    out_refs = (o0_ref, o1_ref, o2_ref, o3_ref)

    @pl.when(pair == 0)
    def _():
        if fetch:
            fetch.start()
        for index, ref in enumerate((z1_ref, z2_ref, z3_ref)):
            x_scr[index * rows : (index + 1) * rows, :] = ref[...]
        tile_scr[...] = jnp.zeros_like(tile_scr)
        kv_scr[0] = project(x_scr[...], wk0_ref, wv0_ref)

    current = pair & 1
    both_lanes = pl.ds(pl.multiple_of(pair * 2 * LANES, LANES), 2 * LANES)
    early = early_ref[2 * sample * rows : 2 * (sample + 1) * rows, both_lanes]
    pairs = jnp.concatenate([kv_scr[current], early], 0)
    keys, values = pairs[:, :LANES], pairs[:, LANES:]
    low_all = lax.broadcasted_iota(jnp.int32, keys.shape, 1) < HEAD_DIM
    zero = jnp.zeros((), BF16)
    one = jnp.ones((), BF16)
    low_values = jnp.concatenate(
        [jnp.where(low_all, values, zero), jnp.where(low_all, one, zero)], axis=1
    )
    high_values = jnp.concatenate(
        [jnp.where(low_all, zero, values), jnp.where(low_all, zero, one)], axis=1
    )
    common, own = slice(0, 3 * rows), slice(4 * rows, 5 * rows)
    lanes = pl.ds(pl.multiple_of(pair * LANES, LANES), LANES)
    mine = q0_ref[part, lanes]
    others = [ref[part, lanes] for ref in (q1_ref, q2_ref, q3_ref)]

    own_keys, other_keys = keys[: 4 * rows], jnp.concatenate([keys[common], keys[own]], 0)
    low_part = lax.broadcasted_iota(jnp.int32, (rows, LANES), 1) < HEAD_DIM
    lows = [jnp.where(low_part, q, zero) for q in (mine, *others)]
    highs = [jnp.where(low_part, zero, q) for q in (mine, *others)]
    scores = [
        (scores_of(part[0], own_keys), scores_of(jnp.concatenate(part[1:], 0), other_keys))
        for part in (lows, highs)
    ]
    tops, sums = [], []
    for (first, rest), head_values in zip(scores, (low_values, high_values)):
        both = jnp.concatenate([first, rest], 0)
        top = jnp.max(both, -1, keepdims=True)
        both = jnp.exp(both - top).astype(BF16)
        tops.append(top)
        sums.append(
            jnp.concatenate(
                [
                    jnp.dot(both[:rows], head_values[: 4 * rows], preferred_element_type=F32),
                    jnp.dot(
                        both[rows:],
                        jnp.concatenate([head_values[common], head_values[own]], 0),
                        preferred_element_type=F32,
                    ),
                ],
                0,
            )
        )
    summed = sums[0] + sums[1]
    total = summed[:, LANES:]
    mixed = (summed[:, :LANES] / total).astype(BF16)
    for index, o_ref in enumerate(out_refs):
        o_ref[:, lanes] = mixed[index * rows : (index + 1) * rows]
    lane = lax.broadcasted_iota(jnp.int32, total.shape, 1)
    logs = jnp.where(lane < HEAD_DIM, tops[0], tops[1]) + jnp.log(total)
    tile_scr[...] = jnp.where((lane & (HEAD_DIM - 1)) == pair, logs, tile_scr[...])
    kv_scr[1 - current] = project(x_scr[...], wk_ref, wv_ref)

    @pl.when(pair == pl.num_programs(0) - 1)
    def _():
        if fetch:
            fetch.wait()
        rest = tile_scr[...]
        tile = jnp.zeros_like(rest)
        for piece in range(3):
            rounded = rest.astype(BF16).astype(F32)
            rest = rest - rounded
            tile = tile + (pltpu.roll(rounded, piece * PIECES, 1) if piece else rounded)
        for index, o_ref in enumerate(out_refs):
            o_ref[:, channels:] = tile[index * rows : (index + 1) * rows].astype(BF16)


def spread_matrix(channels):
    out = np.zeros((LANES, channels), np.float32)
    for channel in range(channels):
        head = channel // HEAD_DIM
        base = (head % 2) * HEAD_DIM + head // 2
        for piece in range(3):
            out[base + piece * PIECES, channel] = 1
    return out


def exact_dot(x, ones):
    total = None
    for _ in range(3):
        rounded = x.astype(BF16)
        part = jnp.dot(rounded, ones, preferred_element_type=F32)
        total = part if total is None else total + part
        x = x - rounded.astype(F32)
    return total


def merge_kernel(*refs):
    *o_refs, hidden_ref, w_ref, spread_ref, gather_ref, res_ref, stat_ref = refs
    channels = hidden_ref.shape[1]
    rows = o_refs[0].shape[0]
    samples = len(o_refs) // 4
    attended = []
    for sample in range(samples):
        parts = o_refs[4 * sample : 4 * sample + 4]
        tiles = jnp.concatenate([ref[:, channels:] for ref in parts], 0)
        logs = jnp.dot(tiles, spread_ref[...], preferred_element_type=F32)
        logs = [logs[index * rows : (index + 1) * rows] for index in range(4)]
        top = jnp.maximum(jnp.maximum(logs[0], logs[1]), jnp.maximum(logs[2], logs[3]))
        numer = denom = None
        for ref, one in zip(parts, logs):
            factor = jnp.exp(one - top)
            upper = factor * ref[:, :channels].astype(F32)
            numer, denom = (upper, factor) if numer is None else (numer + upper, denom + factor)
        attended.append((numer / denom).astype(BF16))
    residual = (
        hidden_ref[...].astype(F32)
        + jnp.dot(jnp.concatenate(attended, 0), w_ref[...], preferred_element_type=F32)
    ).astype(BF16)
    res_ref[...] = residual
    wide = residual.astype(F32)
    sums = []
    for sample in range(samples):
        part = wide[sample * rows : (sample + 1) * rows]
        sums += [jnp.sum(part, 0, keepdims=True), jnp.sum(part * part, 0, keepdims=True)]
    sums = jnp.concatenate(sums + [jnp.zeros((8 - len(sums), channels), F32)], 0)
    stat_ref[...] = exact_dot(sums, gather_ref[...])


def shifted(x, by, cols):
    rolled = pltpu.roll(x, by % x.shape[0], 0)
    col = lax.broadcasted_iota(jnp.int32, x.shape, 0) & (cols - 1)
    edge = 0 if by == 1 else cols - 1
    return jnp.where(col == edge, 0.0, rolled).astype(BF16)


def taps(x, weights, cols):
    wide = x.astype(F32)
    unfolded = jnp.concatenate([shifted(wide, 1, cols), x, shifted(wide, -1, cols)], 1)
    weights = weights.reshape(-1, weights.shape[-1])
    return jnp.dot(unfolded, weights, preferred_element_type=F32)


def above_kernel(x_ref, w_ref, bias_ref, shift_ref, out_ref, *, cols):
    total = taps(x_ref[...], w_ref[0], cols) + as_row(bias_ref)
    for sample in range(total.shape[0] // cols):
        part = slice(sample * cols, (sample + 1) * cols)
        out_ref[part, :] = total[part] + shift_ref[sample : sample + 1, :]


def below_kernel(x_ref, w_ref, above_ref, out_ref, *, cols):
    out_ref[...] = taps(x_ref[...], w_ref[2], cols) + above_ref[...]


def add_kernel(*refs):
    refs[-1][...] = (refs[0][...] + refs[1][...]) + (refs[2][...] + refs[3][...])


def final_kernel(
    res_ref, s0_ref, s1_ref, s2_ref, s3_ref, gain_ref, bias_ref, scatter_ref, w_ref, rim_ref, out_ref,
    *, cols, cells
):
    activated = []
    sums = (s0_ref[...] + s1_ref[...]) + (s2_ref[...] + s3_ref[...])
    sums = exact_dot(sums, scatter_ref[...])
    gain, bias = as_row(gain_ref), as_row(bias_ref)
    wide = res_ref[...].astype(F32)
    for sample in range(wide.shape[0] // cols):
        mean = sums[2 * sample : 2 * sample + 1] / cells
        var = sums[2 * sample + 1 : 2 * sample + 2] / cells - mean * mean
        residual = wide[sample * cols : (sample + 1) * cols]
        normalized = (residual - mean) * lax.rsqrt(var + EPSILON)
        value = normalized * gain + bias
        activated.append((value / (1.0 + jnp.exp(-value))).astype(BF16))
    x = jnp.concatenate(activated, 0)
    out_ref[...] = (
        taps(x, w_ref[1], cols) + rim_ref[...] + wide
    ).astype(BF16)


def ring(by, count):
    return [(i, (i + by) % count) for i in range(count)]


def call(kernel, out_shape, *args, flops=1000000, chip=(), slow=(), **kwargs):
    spaces = {**dict.fromkeys(chip, pltpu.VMEM), **dict.fromkeys(slow, pltpu.HBM)}
    args = [
        pltpu.with_memory_space_constraint(x, spaces[index]) if index in spaces else x
        for index, x in enumerate(args)
    ]
    return pl.pallas_call(
        kernel,
        out_shape=out_shape,
        compiler_params=pltpu.CompilerParams(vmem_limit_bytes=24 * 2 ** 20),
        cost_estimate=pl.CostEstimate(flops=flops, bytes_accessed=1000000, transcendentals=0),
        **kwargs,
    )(*args)


def shards(
    hidden, stale_attn_in, stale_conv_in, ln_gain, ln_bias, w_qkv, w_out,
    gn_gain, gn_bias, conv_weight, conv_bias, time_shift,
):
    samples, rows_dev, cols, channels = hidden.shape
    tokens = rows_dev * cols
    every = samples * tokens
    pair_count = channels // LANES
    y_count, z_count = lax.axis_size("y"), lax.axis_size("z")
    count = y_count * z_count
    hid = hidden.reshape(every, channels)
    block = pltpu.VMEM((tokens, channels), BF16)
    full = pl.BlockSpec((every, channels), lambda i: (0, 0))
    vector = pl.BlockSpec((channels,), lambda i: (0,))
    shifts = (1, 3, 2)

    both = pltpu.VMEM((every, channels), BF16)
    stale = call(
        stale_norm_kernel, [block] * samples,
        stale_attn_in.reshape(every, channels), ln_gain, ln_bias,
        grid=(1,),
        in_specs=[full, vector, vector],
        out_specs=[VMEM] * samples,
        slow=(0, 1, 2),
        flops=6 * 10 ** 9,
    )
    along = []
    for s, one in enumerate(stale):
        up, down = (lax.ppermute(one, "z", ring(by, z_count)) for by in (1, 3))
        far = lax.ppermute(up, "z", ring(1, z_count)) if s % 2 == 0 else lax.ppermute(
            down, "z", ring(3, z_count)
        )
        along.append((up, far, down))
    queries, fresh = call(
        query_kernel, [both] * 2, hid, ln_gain, ln_bias, w_qkv,
        grid=(1,),
        in_specs=[VMEM, VMEM, VMEM, pl.BlockSpec((channels, channels), lambda i: (0, 0))],
        out_specs=[VMEM] * 2,
        flops=6 * 10 ** 9,
    )
    all_queries = [queries] + [lax.ppermute(queries, "y", ring(by, y_count)) for by in shifts]
    early = call(
        early_kernel, pltpu.VMEM((2 * every, 2 * channels), BF16),
        fresh, *stale, w_qkv, w_qkv,
        grid=(pair_count,),
        in_specs=[VMEM] * (1 + samples)
        + [
            pl.BlockSpec((channels, LANES), lambda p: (0, pair_count + p)),
            pl.BlockSpec((channels, LANES), lambda p: (0, 2 * pair_count + p)),
        ],
        out_specs=VMEM,
        scratch_shapes=[pltpu.VMEM((2 * every, channels), BF16)],
        chip=range(1 + samples),
        flops=6 * 10 ** 9,
    )
    conv_rows = stale_conv_in.reshape(every, channels)
    above = lax.ppermute(conv_rows, ("y", "z"), [(i, i + 1) for i in range(count - 1)])
    below = lax.ppermute(conv_rows, ("y", "z"), [(i + 1, i) for i in range(count - 1)])

    wide = channels + LANES
    spread = jnp.asarray(spread_matrix(channels), BF16)
    group = np.arange(channels) // (channels // GROUPS)
    gather = group[:, None] == np.arange(LANES)[None, :]
    ext = pltpu.VMEM((tokens, wide), BF16)
    back = []
    for s in range(samples):
        extra = [pltpu.VMEM(conv_weight.shape, BF16)] * (s == samples - 1)
        outs = call(
            functools.partial(attend_kernel, sample=s), [ext] * 4 + extra,
            *all_queries, *along[s], early,
            w_qkv, w_qkv, w_qkv, w_qkv, conv_weight,
            grid=(pair_count,),
            in_specs=[VMEM] * 8
            + [
                pl.BlockSpec((channels, LANES), lambda p: (0, pair_count)),
                pl.BlockSpec((channels, LANES), lambda p: (0, 2 * pair_count)),
                pl.BlockSpec((channels, LANES), lambda p: (0, jnp.minimum(pair_count + p + 1, 2 * pair_count - 1))),
                pl.BlockSpec((channels, LANES), lambda p: (0, jnp.minimum(2 * pair_count + p + 1, 3 * pair_count - 1))),
                pl.BlockSpec(memory_space=pl.ANY),
            ],
            out_specs=[VMEM] * (4 + len(extra)),
            scratch_shapes=[
                pltpu.VMEM((3 * tokens, channels), BF16),
                pltpu.VMEM((2, 3 * tokens, 2 * LANES), BF16),
                pltpu.VMEM((4 * tokens, LANES), F32),
                pltpu.SemaphoreType.DMA,
            ],
            flops=6 * 10 ** 9,
            chip=range(8),
            slow=(12,),
        )
        back.append(
            [outs[0]]
            + [lax.ppermute(one, "y", ring(-by, y_count)) for one, by in zip(outs[1:4], shifts)]
        )
    conv_on_chip = outs[4]
    rim = pltpu.VMEM((every, channels), F32)
    upper = call(
        functools.partial(above_kernel, cols=cols), rim,
        above, conv_on_chip, conv_bias, time_shift,
        in_specs=[VMEM] * 4, out_specs=VMEM, chip=(0, 1),
        flops=6 * every * channels * channels,
    )
    rim = call(
        functools.partial(below_kernel, cols=cols), rim, below, conv_on_chip, upper,
        in_specs=[VMEM] * 3, out_specs=VMEM, chip=(0, 1, 2),
        flops=6 * every * channels * channels,
    )
    small = pltpu.VMEM((8, LANES), F32)
    residual, stat = call(
        merge_kernel, [both, small],
        *sum(back, []), hid, w_out, spread, jnp.asarray(gather, BF16),
        grid=(1,),
        in_specs=[VMEM] * (4 * samples + 4),
        out_specs=[VMEM, VMEM],
        flops=6 * 10 ** 9,
        chip=tuple(range(4 * samples)) + (4 * samples + 1,),
    )
    along_y = [stat] + [lax.ppermute(stat, "y", ring(by, y_count)) for by in shifts]
    stat = call(add_kernel, small, *along_y, in_specs=[VMEM] * 4, out_specs=VMEM, chip=range(4))
    along_z = [stat] + [lax.ppermute(stat, "z", ring(by, z_count)) for by in shifts]
    out = call(
        functools.partial(
            final_kernel, cols=cols, cells=float(count * tokens * (channels // GROUPS))
        ),
        jax.ShapeDtypeStruct((every, channels), BF16),
        residual, *along_z, gn_gain, gn_bias, jnp.asarray(gather.T, BF16), conv_on_chip, rim,
        in_specs=[VMEM] * 10,
        out_specs=VMEM,
        chip=(0, 1, 2, 3, 4, 8, 9),
        flops=6 * every * channels * channels,
    )
    return out.reshape(hidden.shape)


def solution(mesh):
    split = Mesh(mesh.devices.reshape(mesh.shape["img"], 4, 4), ("img", "y", "z"))
    rows = P("img", ("y", "z"), None, None)

    return jax.shard_map(
        shards,
        mesh=split,
        in_specs=(rows, rows, rows, P(), P(), P(), P(), P(), P(), P(), P(), P("img", None)),
        out_specs=rows,
        check_vma=False,
    )
```
